32 devices in a mesh: dp: 4 (over y, z), tp: 8 (over x, core).
Axes of the slice: x: 4, y: 2, z: 2, core: 2. Of those that a mesh axis runs over, the one named last changes fastest.
The devices are a block of a 4x4x8 slice.
Arguments:
- enc_out: bfloat16 [48, 512, 2048], P('dp', 'tp'), parts along dimension 0
- norm_scale: bfloat16 [2048], replicated
- w_key: bfloat16 [6, 2048, 32, 64], P(None, None, 'tp')
- w_value: bfloat16 [6, 2048, 32, 64], P(None, None, 'tp')
Outputs:
- output 1: bfloat16 [6, 48, 512, 32, 64], P(None, 'dp', None, 'tp'), parts along dimension 1
- output 2: bfloat16 [6, 48, 512, 32, 64], P(None, 'dp', None, 'tp'), parts along dimension 1
There are 4 independent parts. The reference program is written for one: setup_inputs(seed, part) draws one part's arguments, and reference() takes and returns one part's arrays. A program takes and returns all parts, laid end to end along the dimension named above; an argument that names none is the same for every part.
All inputs are finite; a program needn't handle non-finite values.
Results may differ from the reference program's by a relative error of at most 0.001.
Values are sent between devices in bfloat16 or wider.
A program may use at most 768 MiB of HBM per device.

```python
import jax
import jax.numpy as jnp
from jax import lax

N_LAYERS = 6
BATCH_SIZE = 12
SEQ_LEN = 512
D_MODEL = 2048
N_HEADS = 32
HEAD_DIM = 64
NORM_EPS = 1e-6


def setup_inputs(seed: int = 0, part: int = 0) -> dict:
    root_key = jax.random.key(seed)
    k_act, k_norm, k_key, k_val = jax.random.split(root_key, 4)
    k_act = jax.random.fold_in(k_act, part)
    w_scale = D_MODEL ** -0.5
    w_shape = (N_LAYERS, D_MODEL, N_HEADS, HEAD_DIM)
    enc_out = jax.random.normal(k_act, (BATCH_SIZE, SEQ_LEN, D_MODEL), jnp.float32)
    norm_scale = jax.random.uniform(k_norm, (D_MODEL,), jnp.float32, 0.5, 1.5)
    w_key = jax.random.normal(k_key, w_shape, jnp.float32) * w_scale
    w_value = jax.random.normal(k_val, w_shape, jnp.float32) * w_scale
    return {"enc_out": enc_out.astype(jnp.bfloat16), "norm_scale": norm_scale.astype(jnp.bfloat16), "w_key": w_key.astype(jnp.bfloat16), "w_value": w_value.astype(jnp.bfloat16)}


def rms_norm(enc_out, norm_scale):
    acts = enc_out.astype(jnp.float32)
    mean_sq = jnp.mean(acts * acts, axis=-1, keepdims=True)
    return (acts * lax.rsqrt(mean_sq + NORM_EPS) * norm_scale.astype(jnp.float32)).astype(jnp.bfloat16)


def reference(enc_out, norm_scale, w_key, w_value):
    normed = rms_norm(enc_out, norm_scale).reshape(BATCH_SIZE * SEQ_LEN, D_MODEL)
    out_shape = (BATCH_SIZE, SEQ_LEN, N_HEADS, HEAD_DIM)

    def project(layer_weights):
        layer_key, layer_value = layer_weights
        keys = jnp.dot(normed, layer_key.reshape(D_MODEL, N_HEADS * HEAD_DIM), preferred_element_type=jnp.float32)
        values = jnp.dot(normed, layer_value.reshape(D_MODEL, N_HEADS * HEAD_DIM), preferred_element_type=jnp.float32)
        return keys.astype(jnp.bfloat16).reshape(out_shape), values.astype(jnp.bfloat16).reshape(out_shape)

    key_cache, value_cache = lax.map(project, (w_key, w_value))
    return key_cache, value_cache
```

```python
import functools

import jax
import jax.numpy as jnp
from jax import lax
from jax.experimental import pallas as pl
from jax.experimental.pallas import tpu as pltpu
from jax.sharding import PartitionSpec as P


NORM_EPS = 1e-6
PIECE = 2
ANY = pl.BlockSpec(memory_space=pl.ANY)
VMEM = pl.BlockSpec(memory_space=pltpu.VMEM)
NT = (((1,), (1,)), ((), ()))
MESH = pl.DeviceIdType.MESH


def in_hbm(x):
    return pltpu.with_memory_space_constraint(x, pltpu.HBM)


def rms_norm(x, scale):
    acts = x.astype(jnp.float32)
    mean_sq = jnp.mean(acts * acts, axis=-1, keepdims=True)
    return (acts * lax.rsqrt(mean_sq + NORM_EPS) * scale).astype(jnp.bfloat16)


def prep_kernel(slots, n_slots, n_weights, x_ref, scale_ref, *refs):
    w_in, refs = refs[:n_weights], refs[n_weights:]
    outs, refs = refs[:len(slots)], refs[len(slots):]
    w_out, (xbuf, ybuf, scale_buf, in_sem, w_sem, send_sem, recv_sem) = refs[:n_weights], refs[n_weights:]
    half = x_ref.shape[1]
    me = lax.axis_index("tp")
    core = lax.rem(me, 2)
    other = me + 1 - 2 * core
    rows = pl.ds(pl.multiple_of(core * half, half), half)
    shift = n_slots // 2
    needed = [i for i in range(n_slots) if i in slots or (i + shift) % n_slots in slots]

    barrier = pltpu.get_barrier_semaphore()
    pl.semaphore_signal(barrier, inc=1, device_id={"tp": other}, device_id_type=MESH)

    def load(j):
        first = lax.rem(needed[j] + shift * core, n_slots) * PIECE
        return pltpu.make_async_copy(x_ref.at[pl.ds(first, PIECE)], xbuf.at[j], in_sem.at[j])

    def send(j):
        to = slots.index((needed[j] + shift) % n_slots)
        return pltpu.make_async_remote_copy(
            src_ref=ybuf.at[j],
            dst_ref=outs[to].at[:, rows],
            send_sem=send_sem.at[to],
            recv_sem=recv_sem.at[to],
            device_id={"tp": other},
            device_id_type=MESH,
        )

    get_scale = pltpu.make_async_copy(scale_ref, scale_buf, w_sem.at[n_weights])
    get_scale.start()
    for j in range(len(needed)):
        load(j).start()
    weights = [pltpu.make_async_copy(a, b, w_sem.at[i]) for i, (a, b) in enumerate(zip(w_in, w_out))]
    for copy in weights:
        copy.start()
    get_scale.wait()
    scale = scale_buf[...].astype(jnp.float32).reshape(1, -1)
    sent = []
    order = sorted(range(len(needed)), key=lambda j: (needed[j] + shift) % n_slots not in slots)
    pending = None
    pl.semaphore_wait(barrier, 1)
    for j in order:
        load(j).wait()
        y = rms_norm(xbuf[j], scale)
        sends = (needed[j] + shift) % n_slots in slots
        if sends:
            ybuf[j] = y
        if needed[j] in slots:
            outs[slots.index(needed[j])][:, rows] = y
        if pending is not None:
            send(pending).start()
            sent.append(pending)
        pending = j if sends else None
    if pending is not None:
        send(pending).start()
        sent.append(pending)
    for j in sent:
        send(j).wait()
    for copy in weights:
        copy.wait()


def prepare(x, scale, slots, n_slots, weights, collective_id):
    _, half, d = x.shape
    shift = n_slots // 2
    n_needed = len([i for i in range(n_slots) if i in slots or (i + shift) % n_slots in slots])
    piece = jax.ShapeDtypeStruct((PIECE, 2 * half, d), x.dtype)
    out_shape = (piece,) * len(slots) + tuple(jax.ShapeDtypeStruct(w.shape, w.dtype) for w in weights)
    return pl.pallas_call(
        functools.partial(prep_kernel, slots, n_slots, len(weights)),
        out_shape=out_shape,
        in_specs=[ANY, ANY] + [ANY] * len(weights),
        out_specs=(VMEM,) * len(out_shape),
        scratch_shapes=[
            pltpu.VMEM((n_needed, PIECE, half, d), x.dtype),
            pltpu.VMEM((n_needed, PIECE, half, d), x.dtype),
            pltpu.VMEM(scale.shape, scale.dtype),
            pltpu.SemaphoreType.DMA((n_needed,)),
            pltpu.SemaphoreType.DMA((len(weights) + 1,)),
            pltpu.SemaphoreType.DMA((len(slots),)),
            pltpu.SemaphoreType.DMA((len(slots),)),
        ],
        compiler_params=pltpu.CompilerParams(vmem_limit_bytes=32 * 2**20, collective_id=collective_id, has_side_effects=True),
        cost_estimate=pl.CostEstimate(flops=64 * x.size, bytes_accessed=4 * x.size, transcendentals=0),
    )(in_hbm(x), in_hbm(scale), *map(in_hbm, weights))


def project_kernel(plan, n_pieces, n_alias, *refs):
    wk_ref, wv_ref = refs[:2]
    pieces = refs[2:2 + n_pieces]
    ok_ref, ov_ref, stage, sem = refs[2 + n_pieces + n_alias:]
    chips = lax.axis_size("tp") // 2
    me = lax.axis_index("tp")
    core, chip = lax.rem(me, 2), me // 2
    group, d = pieces[0].shape[1:]
    hk = wk_ref.shape[1]
    chunks, _, per = stage.shape[:3]

    def put(i, c):
        copies = []
        at = 0
        for j, (p, on0, on1) in enumerate(plan[i]):
            n = pieces[p].shape[0]
            off, first = (a if a is b else jnp.where(core == 0, a, b) for a, b in zip(on0, on1))
            lanes = pl.ds(pl.multiple_of(lax.rem(chip + off, chips) * group, group), group)
            for kv, out in enumerate((ok_ref, ov_ref)):
                dst = out.at[pl.ds(c * per, per), pl.ds(first, n), :, lanes]
                copies.append(pltpu.make_async_copy(stage.at[c, kv, :, pl.ds(at, n)], dst, sem.at[c, kv, j]))
            at += n
        return copies

    for i, block in enumerate(plan):

        @pl.loop(0, chunks)
        def _(c):
            if i > 0:
                for copy in put(i - 1, c):
                    copy.wait()
            y = jnp.concatenate([pieces[p][...].reshape(-1, d) for p, _, _ in block])
            for kv, w_ref in enumerate((wk_ref, wv_ref)):
                w = w_ref[pl.ds(c * per, per)].reshape(per * hk, d)
                res = lax.dot_general(w, y, NT, preferred_element_type=jnp.float32).astype(jnp.bfloat16)
                for l in range(per):
                    for s in range(y.shape[0] // group):
                        stage[c, kv, l, s] = res[l * hk:(l + 1) * hk, s * group:(s + 1) * group]
            for copy in put(i, c):
                copy.start()

    for c in range(chunks):
        for copy in put(len(plan) - 1, c):
            copy.wait()


def project(wk, wv, blocks, out, batch, tp):
    layers, hk, d = wk.shape
    pieces, plan = [], []
    for block in blocks:
        plan.append(tuple((len(pieces) + j, *where) for j, (_, *where) in enumerate(block)))
        pieces += [piece for piece, *_ in block]
    group = pieces[0].shape[1]
    shape = jax.ShapeDtypeStruct((layers, batch, hk, group * tp // 2), wk.dtype)
    n_alias = 0 if out is None else 2
    n_in = 2 + len(pieces)
    per = 2
    tok = sum(p.shape[0] for p in pieces) * group
    seqs = sum(p.shape[0] for p, *_ in blocks[0])
    return pl.pallas_call(
        functools.partial(project_kernel, tuple(plan), len(pieces), n_alias),
        out_shape=(shape, shape),
        in_specs=[VMEM] * n_in + [ANY] * n_alias,
        out_specs=(ANY, ANY),
        input_output_aliases={n_in + i: i for i in range(n_alias)},
        scratch_shapes=[
            pltpu.VMEM((layers // per, 2, per, seqs, hk, group), wk.dtype),
            pltpu.SemaphoreType.DMA((layers // per, 2, len(blocks[0]))),
        ],
        compiler_params=pltpu.CompilerParams(vmem_limit_bytes=10 * 2**20),
        cost_estimate=pl.CostEstimate(
            flops=2 * tok * d * hk * 2 * layers,
            bytes_accessed=2 * tok * (d + 2 * layers * hk),
            transcendentals=0,
        ),
    )(wk, wv, *pieces, *(out or ()))


def solution(mesh):
    tp = mesh.shape["tp"]
    chips = tp // 2
    ring = [(i, (i + 2 - 4 * (i % 2)) % tp) for i in range(tp)]
    swap = [(i, i ^ 1) for i in range(tp)]

    def send(v, perm):
        return lax.ppermute(v, "tp", perm)

    def per_device(enc_out, norm_scale, w_key, w_value):
        layers, d, heads, k = w_key.shape
        batch = enc_out.shape[0]
        wk = w_key.reshape(layers, d, heads * k).transpose(0, 2, 1)
        wv = w_value.reshape(layers, d, heads * k).transpose(0, 2, 1)
        n = batch // PIECE
        h = n // 2
        seq = lambda i: (i % n) * PIECE

        def run(blocks, out):
            return project(wk, wv, blocks, out, batch, tp)

        def hold(arrays, out):
            return lax.optimization_barrier((tuple(arrays), out))

        s0, = prepare(enc_out, norm_scale, (0,), n, (), 0)
        near = [None] * n
        near[0] = send(s0, ring)
        *rest, wk, wv = prepare(enc_out, norm_scale, tuple(range(1, n)), n, (wk, wv), 1)
        slots = [s0, *rest]
        near[1] = send(slots[1], ring)
        near[2] = send(slots[2], ring)
        own = [(slots[i], (0, seq(i)), (0, seq(i + h))) for i in range(n)]
        out = run([own[0:2], own[2:4]], None)

        def swapped(v):
            return send(v, swap)

        LEFT, RIGHT = chips - 1, 1

        def near_block(i, p, q):
            mine = ((LEFT, seq(i)), (RIGHT, seq(i + h)))
            return [(p, *mine), (q, *mine[::-1])]

        def far_block(i, p, q):
            mine = ((2, seq(i)), (2, seq(i + h)))
            return [(p, *mine), (q, *mine[::-1])]

        far = [None] * h
        (p0, p1), out = hold(near[:2], out)
        q0, q1 = swapped(p0), swapped(p1)
        near[3] = send(slots[3], ring)
        near[4] = send(slots[4], ring)
        out = run([own[4:6]], out)
        (p2,), out = hold(near[2:3], out)
        q2 = swapped(p2)
        near[5] = send(slots[5], ring)
        out = run([near_block(0, p0, q0), near_block(1, p1, q1)], out)
        (p3,), out = hold(near[3:4], out)
        q3 = swapped(p3)
        far[0] = send(p0, ring)
        out = run([near_block(2, p2, q2)], out)
        (p4,), out = hold(near[4:5], out)
        q4 = swapped(p4)
        far[1] = send(p1, ring)
        out = run([near_block(3, p3, q3)], out)
        (p5,), out = hold(near[5:6], out)
        q5 = swapped(p5)
        far[2] = send(p2, ring)
        out = run([near_block(4, p4, q4)], out)
        (p6,), out = hold(far[0:1], out)
        q6 = swapped(p6)
        out = run([near_block(5, p5, q5)], out)
        out = run([far_block(0, p6, q6)], out)
        (p7,), out = hold(far[1:2], out)
        q7 = swapped(p7)
        out = run([far_block(1, p7, q7)], out)
        (p8,), out = hold(far[2:3], out)
        q8 = swapped(p8)
        out = run([far_block(2, p8, q8)], out)
        to_cache = lambda o: o.reshape(layers, batch, heads, k, -1).transpose(0, 1, 4, 2, 3)
        return to_cache(out[0]), to_cache(out[1])

    weight_spec = P(None, None, "tp", None)
    cache_spec = P(None, "dp", None, "tp", None)
    step = jax.shard_map(per_device, mesh=mesh, in_specs=(P("dp", "tp", None), P(None), weight_spec, weight_spec), out_specs=(cache_spec, cache_spec), check_vma=False)

    def program(*args):
        jax.eval_shape(step, *args)
        return step(*args)

    return program
```

```python
import functools

import jax
import jax.numpy as jnp
from jax import lax
from jax.experimental import pallas as pl
from jax.experimental.pallas import tpu as pltpu
from jax.sharding import PartitionSpec as P


NORM_EPS = 1e-6
PIECE = 2
LAYERS = 2
ANY = pl.BlockSpec(memory_space=pl.ANY)
VMEM = pl.BlockSpec(memory_space=pltpu.VMEM)
NT = (((1,), (1,)), ((), ()))
MESH = pl.DeviceIdType.MESH


def in_hbm(x):
    return pltpu.with_memory_space_constraint(x, pltpu.HBM)


def rms_norm(x, scale):
    acts = x.astype(jnp.float32)
    mean_sq = jnp.mean(acts * acts, axis=-1, keepdims=True)
    return (acts * lax.rsqrt(mean_sq + NORM_EPS) * scale).astype(jnp.bfloat16)


def output_copies(outs, stage, sem, entry, c, per):
    chips = lax.axis_size("tp") // 2
    me = lax.axis_index("tp")
    core, chip = lax.rem(me, 2), me // 2
    group = stage.shape[-1]
    copies = []
    at = 0
    for j, (n, on0, on1) in enumerate(entry):
        off, first = (a if a is b else jnp.where(core == 0, a, b) for a, b in zip(on0, on1))
        lanes = pl.ds(pl.multiple_of(lax.rem(chip + off, chips) * group, group), group)
        for kv, out in enumerate(outs):
            dst = out.at[pl.ds(c * per, per), pl.ds(first, n), :, lanes]
            copies.append(pltpu.make_async_copy(stage.at[c, kv, :, pl.ds(at, n)], dst, sem.at[c, kv, j]))
        at += n
    return copies


def matmul_block(w_refs, pieces, stage, c):
    per, _, hk, group = stage.shape[2:]
    d = w_refs[0].shape[-1]
    tokens = [p[...].reshape(-1, d) for p in pieces]
    y = jnp.concatenate(tokens) if len(tokens) > 1 else tokens[0]
    for kv, w_ref in enumerate(w_refs):
        w = w_ref[pl.ds(c * per, per)].reshape(per * hk, d)
        res = lax.dot_general(w, y, NT, preferred_element_type=jnp.float32).astype(stage.dtype)
        for l in range(per):
            for s in range(y.shape[0] // group):
                stage[c, kv, l, s] = res[l * hk:(l + 1) * hk, s * group:(s + 1) * group]


def prep_kernel(slots, n_slots, early, n_weights, x_ref, scale_ref, *refs):
    w_in, refs = refs[:n_weights], refs[n_weights:]
    made, refs = refs[:early], refs[early:]
    outs, refs = refs[:len(slots)], refs[len(slots):]
    w_out, refs = refs[:n_weights], refs[n_weights:]
    stage, refs = (refs[0], refs[1:]) if n_weights else (None, refs)
    xbuf, scale_buf, in_sem, scale_sem, w_sem, send_sem, recv_sem = refs
    half = x_ref.shape[1]
    me = lax.axis_index("tp")
    core = lax.rem(me, 2)
    other = me + 1 - 2 * core
    rows = pl.ds(pl.multiple_of(core * half, half), half)
    shift = n_slots // 2
    there = lambda i: (i + shift) % n_slots
    needed = sorted((i for i in range(n_slots) if i in slots or there(i) in slots), key=lambda i: (slots.index(there(i)) if there(i) in slots else n_slots))

    barrier = pltpu.get_barrier_semaphore()
    pl.semaphore_signal(barrier, inc=1, device_id={"tp": other}, device_id_type=MESH)

    def load(j):
        first = lax.rem(needed[j] + shift * core, n_slots) * PIECE
        return pltpu.make_async_copy(x_ref.at[pl.ds(first, PIECE)], xbuf.at[j], in_sem.at[j])

    def send(j):
        to = slots.index(there(needed[j]))
        return pltpu.make_async_remote_copy(
            src_ref=xbuf.at[j],
            dst_ref=outs[to].at[:, rows],
            send_sem=send_sem.at[to],
            recv_sem=recv_sem.at[to],
            device_id={"tp": other},
            device_id_type=MESH,
        )

    def load_weights(kv, c):
        layers = pl.ds(c * stage.shape[2], stage.shape[2])
        return pltpu.make_async_copy(w_in[kv].at[layers], w_out[kv].at[layers], w_sem.at[kv, c])

    get_scale = pltpu.make_async_copy(scale_ref, scale_buf, scale_sem)
    get_scale.start()
    for j in range(len(needed)):
        load(j).start()
    for c in range(stage.shape[0] if n_weights else 0):
        for kv in range(n_weights):
            load_weights(kv, c).start()
    get_scale.wait()
    scale = scale_buf[...].astype(jnp.float32).reshape(1, -1)
    pending = None
    sent = []
    pl.semaphore_wait(barrier, 1)
    for j, i in enumerate(needed):
        load(j).wait()
        y = rms_norm(xbuf[j], scale)
        if there(i) in slots:
            xbuf[j] = y
        if i in slots:
            outs[slots.index(i)][:, rows] = y
        if pending is not None:
            send(pending).start()
            sent.append(pending)
        pending = j if there(i) in slots else None
    if pending is not None:
        send(pending).start()
        sent.append(pending)
    if n_weights:
        first = sent[0]
        send(first).wait_recv()

        @pl.loop(0, stage.shape[0])
        def _(c):
            for kv in range(n_weights):
                load_weights(kv, c).wait()
            matmul_block(w_out, [*made, outs[slots.index(there(needed[first]))]], stage, c)

    for j in sent:
        send(j).wait_send()
        if not n_weights or j != first:
            send(j).wait_recv()


def stage_shape(weights, seqs, group):
    layers, hk, _ = weights[0].shape
    return jax.ShapeDtypeStruct((layers // LAYERS, len(weights), LAYERS, seqs, hk, group), weights[0].dtype)


def prepare(x, scale, slots, n_slots, early, weights, collective_id):
    _, half, d = x.shape
    shift = n_slots // 2
    n_needed = len([i for i in range(n_slots) if i in slots or (i + shift) % n_slots in slots])
    piece = jax.ShapeDtypeStruct((PIECE, 2 * half, d), x.dtype)
    out_shape = (piece,) * len(slots) + tuple(jax.ShapeDtypeStruct(w.shape, w.dtype) for w in weights)
    if weights:
        out_shape += (stage_shape(weights, PIECE * (len(early) + 1), 2 * half),)
    return pl.pallas_call(
        functools.partial(prep_kernel, slots, n_slots, len(early), len(weights)),
        out_shape=out_shape,
        in_specs=[ANY, ANY] + [ANY] * len(weights) + [VMEM] * len(early),
        out_specs=(VMEM,) * len(out_shape),
        scratch_shapes=[
            pltpu.VMEM((n_needed, PIECE, half, d), x.dtype),
            pltpu.VMEM(scale.shape, scale.dtype),
            pltpu.SemaphoreType.DMA((n_needed,)),
            pltpu.SemaphoreType.DMA,
            pltpu.SemaphoreType.DMA((2, weights[0].shape[0] // LAYERS if weights else 1)),
            pltpu.SemaphoreType.DMA((len(slots),)),
            pltpu.SemaphoreType.DMA((len(slots),)),
        ],
        compiler_params=pltpu.CompilerParams(vmem_limit_bytes=8 * 2**20, collective_id=collective_id, has_side_effects=True),
        cost_estimate=pl.CostEstimate(flops=64 * x.size, bytes_accessed=4 * x.size, transcendentals=0),
    )(in_hbm(x), in_hbm(scale), *map(in_hbm, weights), *early)


def project_kernel(plan, n_pieces, carried, n_alias, keep, *refs):
    w_refs, refs = refs[:2], refs[2:]
    pieces, refs = refs[:n_pieces], refs[n_pieces:]
    before, refs = refs[0], refs[1 + n_alias:]
    outs, stage, refs = refs[:2], refs[2], refs[3:]
    sem, before_sem = refs
    chunks, _, per = stage.shape[:3]
    entry, old_chunks = carried
    late = [copy for c in old_chunks for copy in output_copies(outs, before, before_sem, entry, c, per)]
    for copy in late:
        copy.start()
    put = lambda i, c: output_copies(outs, stage, sem, plan[i], c, per)
    used = 0
    for i, block in enumerate(plan):
        mine = pieces[used:used + len(block)]
        used += len(block)
        last = i == len(plan) - 1 and keep

        @pl.loop(0, chunks)
        def _(c):
            if i > 0:
                for copy in put(i - 1, c):
                    copy.wait()
            matmul_block(w_refs, mine, stage, c)
            if last:

                @pl.when(c < chunks - 1)
                def _():
                    for copy in put(i, c):
                        copy.start()
            else:
                for copy in put(i, c):
                    copy.start()

    for copy in late:
        copy.wait()
    for c in range(chunks - 1 if keep else chunks):
        for copy in put(len(plan) - 1, c):
            copy.wait()


def project(weights, blocks, out, carry, batch, tp, keep):
    layers, hk, d = weights[0].shape
    plan = tuple(tuple((p.shape[0], *where) for p, *where in block) for block in blocks)
    pieces = [piece for block in blocks for piece, *_ in block]
    group = pieces[0].shape[1]
    shape = jax.ShapeDtypeStruct((layers, batch, hk, group * tp // 2), weights[0].dtype)
    n_alias = 0 if out is None else 2
    n_in = 3 + len(pieces)
    stage = stage_shape(weights, sum(n for n, *_ in plan[0]), group)
    before, entry, chunks = carry
    tok = sum(p.shape[0] for p in pieces) * group
    *out, stage_out = pl.pallas_call(
        functools.partial(project_kernel, plan, len(pieces), (entry, chunks), n_alias, keep),
        out_shape=(shape, shape, stage),
        in_specs=[VMEM] * n_in + [ANY] * n_alias,
        out_specs=(ANY, ANY, VMEM),
        input_output_aliases={n_in + i: i for i in range(n_alias)},
        scratch_shapes=[
            pltpu.SemaphoreType.DMA((stage.shape[0], 2, len(plan[0]))),
            pltpu.SemaphoreType.DMA((stage.shape[0], 2, len(entry))),
        ],
        compiler_params=pltpu.CompilerParams(vmem_limit_bytes=4 * 2**20),
        cost_estimate=pl.CostEstimate(
            flops=2 * tok * d * hk * 2 * layers,
            bytes_accessed=2 * tok * (d + 2 * layers * hk),
            transcendentals=0,
        ),
    )(*weights, *pieces, before, *(out or ()))
    return out, (stage_out, plan[-1], (stage.shape[0] - 1,))


def solution(mesh):
    tp = mesh.shape["tp"]
    chips = tp // 2
    ring = [(i, (i + 2 - 4 * (i % 2)) % tp) for i in range(tp)]
    swap = [(i, i ^ 1) for i in range(tp)]

    def send(v, perm):
        return lax.ppermute(v, "tp", perm)

    def per_device(enc_out, norm_scale, w_key, w_value):
        layers, d, heads, k = w_key.shape
        batch = enc_out.shape[0]
        wk = w_key.reshape(layers, d, heads * k).transpose(0, 2, 1)
        wv = w_value.reshape(layers, d, heads * k).transpose(0, 2, 1)
        n = batch // PIECE
        h = n // 2
        seq = lambda i: (i % n) * PIECE

        state = {"out": None}

        def run(blocks, keep=True):
            state["out"], state["carry"] = project(weights, blocks, state["out"], state["carry"], batch, tp, keep)

        def hold(*arrays):
            arrays, state["out"] = lax.optimization_barrier((arrays, state["out"]))
            return arrays if len(arrays) > 1 else arrays[0]

        s0, = prepare(enc_out, norm_scale, (0,), n, (), (), 0)
        n0 = send(s0, ring)
        *rest, wk, wv, stage = prepare(enc_out, norm_scale, tuple(range(1, n)), n, (s0,), (wk, wv), 1)
        weights = (wk, wv)
        slots = [s0, *rest]
        own = [(slots[i], (0, seq(i)), (0, seq(i + h))) for i in range(n)]
        entry = tuple((PIECE, *where) for _, *where in own[:2])
        state["carry"] = (stage, entry, tuple(range(stage.shape[0])))
        n1 = send(slots[1], ring)
        n2 = send(slots[2], ring)
        run([own[2:4]])

        LEFT, RIGHT = chips - 1, 1
        near = lambda i: ((LEFT, seq(i)), (RIGHT, seq(i + h)))
        far = lambda i: ((2, seq(i)), (2, seq(i + h)))
        mine = lambda p, where: (p, *where)
        theirs = lambda q, where: (q, *where[::-1])

        p0 = hold(n0)
        q0 = send(p0, swap)
        n3, n4, n5 = (send(slots[i], ring) for i in range(3, 6))
        run([own[4:6]])
        p1 = hold(n1)
        q1 = send(p1, swap)
        run([[mine(p0, near(0)), theirs(q0, near(0))]])
        p2 = hold(n2)
        q2 = send(p2, swap)
        f0, f1, f2 = (send(p, ring) for p in (p0, p1, p2))
        run([[mine(p1, near(1)), theirs(q1, near(1))]])
        p3 = hold(n3)
        q3 = send(p3, swap)
        run([[mine(p2, near(2)), theirs(q2, near(2))]])
        run([[mine(p3, near(3)), theirs(q3, near(3))]])
        for i, v, where in ((4, n4, near(4)), (5, n5, near(5)), (6, f0, far(0)), (7, f1, far(1)), (8, f2, far(2))):
            p = hold(v)
            q = send(p, swap)
            run([[mine(p, where)]])
            q = hold(q)
            run([[theirs(q, where)]], keep=i < 8)
        out = state["out"]
        to_cache = lambda o: o.reshape(layers, batch, heads, k, -1).transpose(0, 1, 4, 2, 3)
        return to_cache(out[0]), to_cache(out[1])

    weight_spec = P(None, None, "tp", None)
    cache_spec = P(None, "dp", None, "tp", None)
    step = jax.shard_map(per_device, mesh=mesh, in_specs=(P("dp", "tp", None), P(None), weight_spec, weight_spec), out_specs=(cache_spec, cache_spec), check_vma=False)

    def program(*args):
        jax.eval_shape(step, *args)
        return step(*args)

    return program
```

```python
import functools

import jax
import jax.numpy as jnp
from jax import lax
from jax.experimental import pallas as pl
from jax.experimental.pallas import tpu as pltpu
from jax.sharding import PartitionSpec as P


NORM_EPS = 1e-6
PIECE = 2
LAYERS = 2
ANY = pl.BlockSpec(memory_space=pl.ANY)
VMEM = pl.BlockSpec(memory_space=pltpu.VMEM)
NT = (((1,), (1,)), ((), ()))
MESH = pl.DeviceIdType.MESH


def in_hbm(x):
    return pltpu.with_memory_space_constraint(x, pltpu.HBM)


def rms_norm(x, scale):
    acts = x.astype(jnp.float32)
    mean_sq = jnp.mean(acts * acts, axis=-1, keepdims=True)
    return (acts * lax.rsqrt(mean_sq + NORM_EPS) * scale).astype(jnp.bfloat16)


def output_copies(outs, stage, sem, entry, c, per):
    chips = lax.axis_size("tp") // 2
    me = lax.axis_index("tp")
    core, chip = lax.rem(me, 2), me // 2
    group = stage.shape[-1]
    copies = []
    at = 0
    for j, (n, on0, on1) in enumerate(entry):
        off, first = (a if a is b else jnp.where(core == 0, a, b) for a, b in zip(on0, on1))
        lanes = pl.ds(pl.multiple_of(lax.rem(chip + off, chips) * group, group), group)
        for kv, out in enumerate(outs):
            dst = out.at[pl.ds(c * per, per), pl.ds(first, n), :, lanes]
            copies.append(pltpu.make_async_copy(stage.at[c, kv, :, pl.ds(at, n)], dst, sem.at[c, kv, j]))
        at += n
    return copies


def matmul_block(w_refs, pieces, stage, c):
    per, _, hk, group = stage.shape[2:]
    d = w_refs[0].shape[-1]
    tokens = [p[...].reshape(-1, d) for p in pieces]
    y = jnp.concatenate(tokens) if len(tokens) > 1 else tokens[0]
    for kv, w_ref in enumerate(w_refs):
        w = w_ref[pl.ds(c * per, per)].reshape(per * hk, d)
        res = lax.dot_general(w, y, NT, preferred_element_type=jnp.float32).astype(stage.dtype)
        for l in range(per):
            for s in range(y.shape[0] // group):
                stage[c, kv, l, s] = res[l * hk:(l + 1) * hk, s * group:(s + 1) * group]


def prep_kernel(slots, n_slots, early, n_weights, x_ref, scale_ref, *refs):
    w_in, refs = refs[:n_weights], refs[n_weights:]
    made, refs = refs[:early], refs[early:]
    outs, refs = refs[:len(slots)], refs[len(slots):]
    w_out, refs = refs[:n_weights], refs[n_weights:]
    stage, refs = (refs[0], refs[1:]) if n_weights else (None, refs)
    xbuf, scale_buf, in_sem, scale_sem, w_sem, send_sem, recv_sem = refs
    half = x_ref.shape[1]
    me = lax.axis_index("tp")
    core = lax.rem(me, 2)
    other = me + 1 - 2 * core
    rows = pl.ds(pl.multiple_of(core * half, half), half)
    shift = n_slots // 2
    there = lambda i: (i + shift) % n_slots
    needed = sorted((i for i in range(n_slots) if i in slots or there(i) in slots), key=lambda i: (slots.index(there(i)) if there(i) in slots else n_slots))

    barrier = pltpu.get_barrier_semaphore()
    pl.semaphore_signal(barrier, inc=1, device_id={"tp": other}, device_id_type=MESH)

    def load(j):
        first = lax.rem(needed[j] + shift * core, n_slots) * PIECE
        return pltpu.make_async_copy(x_ref.at[pl.ds(first, PIECE)], xbuf.at[j], in_sem.at[j])

    def send(j):
        to = slots.index(there(needed[j]))
        return pltpu.make_async_remote_copy(
            src_ref=xbuf.at[j],
            dst_ref=outs[to].at[:, rows],
            send_sem=send_sem.at[to],
            recv_sem=recv_sem.at[to],
            device_id={"tp": other},
            device_id_type=MESH,
        )

    def load_weights(kv, c):
        layers = pl.ds(c * stage.shape[2], stage.shape[2])
        return pltpu.make_async_copy(w_in[kv].at[layers], w_out[kv].at[layers], w_sem.at[kv, c])

    get_scale = pltpu.make_async_copy(scale_ref, scale_buf, scale_sem)
    get_scale.start()
    for j in range(len(needed)):
        load(j).start()
    for c in range(stage.shape[0] if n_weights else 0):
        for kv in range(n_weights):
            load_weights(kv, c).start()
    get_scale.wait()
    scale = scale_buf[...].astype(jnp.float32).reshape(1, -1)
    pending = None
    sent = []
    pl.semaphore_wait(barrier, 1)
    for j, i in enumerate(needed):
        load(j).wait()
        y = rms_norm(xbuf[j], scale)
        if there(i) in slots:
            xbuf[j] = y
        if i in slots:
            outs[slots.index(i)][:, rows] = y
        if pending is not None:
            send(pending).start()
            sent.append(pending)
        pending = j if there(i) in slots else None
    if pending is not None:
        send(pending).start()
        sent.append(pending)
    if n_weights:

        @pl.loop(0, stage.shape[0])
        def _(c):
            for kv in range(n_weights):
                load_weights(kv, c).wait()
            matmul_block(w_out, made, stage, c)

    for j in sent:
        send(j).wait()


def stage_shape(weights, seqs, group):
    layers, hk, _ = weights[0].shape
    return jax.ShapeDtypeStruct((layers // LAYERS, len(weights), LAYERS, seqs, hk, group), weights[0].dtype)


def prepare(x, scale, slots, n_slots, early, weights, collective_id):
    _, half, d = x.shape
    shift = n_slots // 2
    n_needed = len([i for i in range(n_slots) if i in slots or (i + shift) % n_slots in slots])
    piece = jax.ShapeDtypeStruct((PIECE, 2 * half, d), x.dtype)
    out_shape = (piece,) * len(slots) + tuple(jax.ShapeDtypeStruct(w.shape, w.dtype) for w in weights)
    if weights:
        out_shape += (stage_shape(weights, PIECE * len(early), 2 * half),)
    return pl.pallas_call(
        functools.partial(prep_kernel, slots, n_slots, len(early), len(weights)),
        out_shape=out_shape,
        in_specs=[ANY, ANY] + [ANY] * len(weights) + [VMEM] * len(early),
        out_specs=(VMEM,) * len(out_shape),
        scratch_shapes=[
            pltpu.VMEM((n_needed, PIECE, half, d), x.dtype),
            pltpu.VMEM(scale.shape, scale.dtype),
            pltpu.SemaphoreType.DMA((n_needed,)),
            pltpu.SemaphoreType.DMA,
            pltpu.SemaphoreType.DMA((2, weights[0].shape[0] // LAYERS if weights else 1)),
            pltpu.SemaphoreType.DMA((len(slots),)),
            pltpu.SemaphoreType.DMA((len(slots),)),
        ],
        compiler_params=pltpu.CompilerParams(vmem_limit_bytes=8 * 2**20, collective_id=collective_id, has_side_effects=True),
        cost_estimate=pl.CostEstimate(flops=64 * x.size, bytes_accessed=4 * x.size, transcendentals=0),
    )(in_hbm(x), in_hbm(scale), *map(in_hbm, weights), *early)


def project_kernel(plan, n_pieces, carried, n_alias, keep, *refs):
    w_refs, refs = refs[:2], refs[2:]
    pieces, refs = refs[:n_pieces], refs[n_pieces:]
    before, refs = refs[0], refs[1 + n_alias:]
    outs, (stage, sem, before_sem) = refs[:2], refs[2:]
    chunks, _, per = stage.shape[:3]
    entry, old_chunks = carried
    late = [copy for c in old_chunks for copy in output_copies(outs, before, before_sem, entry, c, per)]
    for copy in late:
        copy.start()
    put = lambda i, c: output_copies(outs, stage, sem, plan[i], c, per)
    used = 0
    for i, block in enumerate(plan):
        mine = pieces[used:used + len(block)]
        used += len(block)
        last = i == len(plan) - 1 and keep

        @pl.loop(0, chunks)
        def _(c):
            if i > 0:
                for copy in put(i - 1, c):
                    copy.wait()
            matmul_block(w_refs, mine, stage, c)
            if last:

                @pl.when(c < chunks - 1)
                def _():
                    for copy in put(i, c):
                        copy.start()
            else:
                for copy in put(i, c):
                    copy.start()

    for copy in late:
        copy.wait()
    for c in range(chunks - 1 if keep else chunks):
        for copy in put(len(plan) - 1, c):
            copy.wait()


def project(weights, blocks, out, carry, batch, tp, keep):
    layers, hk, d = weights[0].shape
    plan = tuple(tuple((p.shape[0], *where) for p, *where in block) for block in blocks)
    pieces = [piece for block in blocks for piece, *_ in block]
    group = pieces[0].shape[1]
    shape = jax.ShapeDtypeStruct((layers, batch, hk, group * tp // 2), weights[0].dtype)
    n_alias = 0 if out is None else 2
    n_in = 3 + len(pieces)
    stage = stage_shape(weights, sum(n for n, *_ in plan[0]), group)
    before, entry, chunks = carry
    tok = sum(p.shape[0] for p in pieces) * group
    *out, = pl.pallas_call(
        functools.partial(project_kernel, plan, len(pieces), (entry, chunks), n_alias, keep),
        out_shape=(shape, shape) + (stage,) * keep,
        in_specs=[VMEM] * n_in + [ANY] * n_alias,
        out_specs=(ANY, ANY) + (VMEM,) * keep,
        input_output_aliases={n_in + i: i for i in range(n_alias)},
        scratch_shapes=[pltpu.VMEM(stage.shape, stage.dtype)] * (not keep) + [
            pltpu.SemaphoreType.DMA((stage.shape[0], 2, len(plan[0]))),
            pltpu.SemaphoreType.DMA((stage.shape[0], 2, len(entry))),
        ],
        compiler_params=pltpu.CompilerParams(vmem_limit_bytes=4 * 2**20),
        cost_estimate=pl.CostEstimate(
            flops=2 * tok * d * hk * 2 * layers,
            bytes_accessed=2 * tok * (d + 2 * layers * hk),
            transcendentals=0,
        ),
    )(*weights, *pieces, before, *(out or ()))
    return out[:2], (out[-1], plan[-1], (stage.shape[0] - 1,))


def solution(mesh):
    tp = mesh.shape["tp"]
    chips = tp // 2
    ring = [(i, (i + 2 - 4 * (i % 2)) % tp) for i in range(tp)]
    swap = [(i, i ^ 1) for i in range(tp)]

    def send(v, perm):
        return lax.ppermute(v, "tp", perm)

    def per_device(enc_out, norm_scale, w_key, w_value):
        layers, d, heads, k = w_key.shape
        batch = enc_out.shape[0]
        wk = w_key.reshape(layers, d, heads * k).transpose(0, 2, 1)
        wv = w_value.reshape(layers, d, heads * k).transpose(0, 2, 1)
        n = batch // PIECE
        h = n // 2
        seq = lambda i: (i % n) * PIECE

        state = {"out": None}

        def run(blocks, keep=True):
            state["out"], state["carry"] = project(weights, blocks, state["out"], state["carry"], batch, tp, keep)

        def hold(*arrays):
            arrays, state["out"] = lax.optimization_barrier((arrays, state["out"]))
            return arrays if len(arrays) > 1 else arrays[0]

        s0, s1 = prepare(enc_out, norm_scale, (0, 1), n, (), (), 0)
        n0, n1 = send(s0, ring), send(s1, ring)
        *rest, wk, wv, stage = prepare(enc_out, norm_scale, tuple(range(2, n)), n, (s0, s1), (wk, wv), 1)
        weights = (wk, wv)
        slots = [s0, s1, *rest]
        own = [(slots[i], (0, seq(i)), (0, seq(i + h))) for i in range(n)]
        entry = tuple((PIECE, *where) for _, *where in own[:2])
        state["carry"] = (stage, entry, tuple(range(stage.shape[0])))
        n2, n3 = send(slots[2], ring), send(slots[3], ring)
        run([own[2:4]])

        LEFT, RIGHT = chips - 1, 1
        near = lambda i: ((LEFT, seq(i)), (RIGHT, seq(i + h)))
        far = lambda i: ((2, seq(i)), (2, seq(i + h)))
        mine = lambda p, where: (p, *where)
        theirs = lambda q, where: (q, *where[::-1])

        p0 = hold(n0)
        q0 = send(p0, swap)
        run([own[4:6]])
        p1 = hold(n1)
        n4, n5 = send(slots[4], ring), send(slots[5], ring)
        q1 = send(p1, swap)
        run([[mine(p0, near(0)), theirs(q0, near(0))]])
        p2 = hold(n2)
        q2 = send(p2, swap)
        run([[mine(p1, near(1)), theirs(q1, near(1))]])
        p3 = hold(n3)
        q3 = send(p3, swap)
        run([[mine(p2, near(2)), theirs(q2, near(2))]])
        p0, p1, p2 = hold(p0, p1, p2)
        f0, f1, f2 = (send(p, ring) for p in (p0, p1, p2))
        run([[mine(p3, near(3)), theirs(q3, near(3))]])
        for i, v, where in ((4, n4, near(4)), (5, n5, near(5)), (6, f0, far(0)), (7, f1, far(1)), (8, f2, far(2))):
            p = hold(v)
            q = send(p, swap)
            run([[mine(p, where)]])
            q = hold(q)
            run([[theirs(q, where)]], keep=i < 8)
        out = state["out"]
        to_cache = lambda o: o.reshape(layers, batch, heads, k, -1).transpose(0, 1, 4, 2, 3)
        return to_cache(out[0]), to_cache(out[1])

    weight_spec = P(None, None, "tp", None)
    cache_spec = P(None, "dp", None, "tp", None)
    step = jax.shard_map(per_device, mesh=mesh, in_specs=(P("dp", "tp", None), P(None), weight_spec, weight_spec), out_specs=(cache_spec, cache_spec), check_vma=False)

    def program(*args):
        jax.eval_shape(step, *args)
        return step(*args)

    return program
```

```python
import functools

import jax
import jax.numpy as jnp
from jax import lax
from jax.experimental import pallas as pl
from jax.experimental.pallas import tpu as pltpu
from jax.sharding import PartitionSpec as P


NORM_EPS = 1e-6
PIECE = 2
LAYERS = 2
ANY = pl.BlockSpec(memory_space=pl.ANY)
VMEM = pl.BlockSpec(memory_space=pltpu.VMEM)
NT = (((1,), (1,)), ((), ()))
MESH = pl.DeviceIdType.MESH


def in_hbm(x):
    return pltpu.with_memory_space_constraint(x, pltpu.HBM)


def rms_norm(x, scale):
    acts = x.astype(jnp.float32)
    mean_sq = jnp.mean(acts * acts, axis=-1, keepdims=True)
    return (acts * lax.rsqrt(mean_sq + NORM_EPS) * scale).astype(jnp.bfloat16)


def output_copies(outs, stage, sem, entry, c, per):
    chips = lax.axis_size("tp") // 2
    me = lax.axis_index("tp")
    core, chip = lax.rem(me, 2), me // 2
    group = stage.shape[-1]
    copies = []
    at = 0
    for j, (n, on0, on1) in enumerate(entry):
        off, first = (a if a is b else jnp.where(core == 0, a, b) for a, b in zip(on0, on1))
        lanes = pl.ds(pl.multiple_of(lax.rem(chip + off, chips) * group, group), group)
        for kv, out in enumerate(outs):
            dst = out.at[pl.ds(c * per, per), pl.ds(first, n), :, lanes]
            copies.append(pltpu.make_async_copy(stage.at[c, kv, :, pl.ds(at, n)], dst, sem.at[c, kv, j]))
        at += n
    return copies


def matmul_block(w_refs, pieces, stage, c):
    per, _, hk, group = stage.shape[2:]
    d = w_refs[0].shape[-1]
    tokens = [p[...].reshape(-1, d) for p in pieces]
    y = jnp.concatenate(tokens) if len(tokens) > 1 else tokens[0]
    for kv, w_ref in enumerate(w_refs):
        w = w_ref[pl.ds(c * per, per)].reshape(per * hk, d)
        res = lax.dot_general(w, y, NT, preferred_element_type=jnp.float32).astype(stage.dtype)
        for l in range(per):
            for s in range(y.shape[0] // group):
                stage[c, kv, l, s] = res[l * hk:(l + 1) * hk, s * group:(s + 1) * group]


def first_kernel(x_ref, scale_ref, y_ref, xbuf, scale_buf, sem, scale_sem):
    n = y_ref.shape[0]
    start = lax.rem(lax.axis_index("tp"), 2) * n
    load = lambda i: pltpu.make_async_copy(x_ref.at[pl.ds(start + i, 1)], xbuf.at[pl.ds(i, 1)], sem.at[i])
    get_scale = pltpu.make_async_copy(scale_ref, scale_buf, scale_sem)
    get_scale.start()
    for i in range(n):
        load(i).start()
    get_scale.wait()
    scale = scale_buf[...].astype(jnp.float32).reshape(1, -1)
    for i in range(n):
        load(i).wait()
        y_ref[i] = rms_norm(xbuf[i], scale)


def normalize_first(x, scale):
    batch, half, d = x.shape
    n = batch // 2
    return pl.pallas_call(
        first_kernel,
        out_shape=jax.ShapeDtypeStruct((n, half, d), x.dtype),
        in_specs=[ANY, ANY],
        out_specs=VMEM,
        scratch_shapes=[
            pltpu.VMEM((n, half, d), x.dtype),
            pltpu.VMEM(scale.shape, scale.dtype),
            pltpu.SemaphoreType.DMA((n,)),
            pltpu.SemaphoreType.DMA,
        ],
        compiler_params=pltpu.CompilerParams(vmem_limit_bytes=8 * 2**20),
        cost_estimate=pl.CostEstimate(flops=32 * x.size, bytes_accessed=2 * x.size, transcendentals=0),
        name="first",
    )(in_hbm(x), in_hbm(scale))


def join(joined, mine, first, theirs):
    n, half = theirs.shape[:2]
    core = lax.rem(lax.axis_index("tp"), 2)
    for s in range(n):
        joined[s, pl.ds(pl.multiple_of(core * half, half), half)] = mine[first + s]
        joined[s, pl.ds(pl.multiple_of((1 - core) * half, half), half)] = theirs[s]


def second_kernel(n_slots, x_ref, scale_ref, wk_ref, wv_ref, y_ref, *refs):
    theirs, refs = refs[:n_slots], refs[n_slots:]
    slots, refs = refs[:n_slots], refs[n_slots:]
    wk_out, wv_out, stage, xbuf, block, scale_buf, in_sem, scale_sem, w_sem, send_sem, recv_sem = refs
    half = x_ref.shape[1]
    me = lax.axis_index("tp")
    core = lax.rem(me, 2)
    other = me + 1 - 2 * core
    rows = pl.ds(pl.multiple_of(core * half, half), half)
    start = (1 - core) * n_slots * PIECE

    barrier = pltpu.get_barrier_semaphore()
    pl.semaphore_signal(barrier, inc=1, device_id={"tp": other}, device_id_type=MESH)

    def load(i):
        return pltpu.make_async_copy(x_ref.at[pl.ds(start + i * PIECE, PIECE)], xbuf.at[i], in_sem.at[i])

    def send(i, src, dst):
        return pltpu.make_async_remote_copy(
            src_ref=src,
            dst_ref=dst,
            send_sem=send_sem.at[i],
            recv_sem=recv_sem.at[i],
            device_id={"tp": other},
            device_id_type=MESH,
        )

    def load_weights(c):
        layers = pl.ds(c * LAYERS, LAYERS)
        pairs = ((wk_ref, wk_out), (wv_ref, wv_out))
        return [pltpu.make_async_copy(a.at[layers], b.at[layers], w_sem.at[kv, c]) for kv, (a, b) in enumerate(pairs)]

    get_scale = pltpu.make_async_copy(scale_ref, scale_buf, scale_sem)
    get_scale.start()
    for i in range(n_slots):
        load(i).start()
    for copy in load_weights(0):
        copy.start()
    to_theirs = [send(i, xbuf.at[i], theirs[i]) for i in range(n_slots)]
    to_slots = [send(n_slots + i, y_ref.at[pl.ds(i * PIECE, PIECE)], slots[i].at[:, rows]) for i in range(n_slots)]
    get_scale.wait()
    scale = scale_buf[...].astype(jnp.float32).reshape(1, -1)
    pl.semaphore_wait(barrier, 1)
    for i in range(n_slots):
        load(i).wait()
        y = rms_norm(xbuf[i], scale)
        xbuf[i] = y
        slots[i][:, rows] = y
        if i > 0:
            to_theirs[i - 1].start()
    for copy in to_slots:
        copy.start()
    to_theirs[-1].start()
    parts = block.shape[0]
    for i in range(parts):
        to_theirs[i].wait_recv()
        join(block.at[i], y_ref, i * PIECE, theirs[i])
    chunks = stage.shape[0]

    @pl.loop(0, chunks)
    def _(c):

        @pl.when(c + 1 < chunks)
        def _():
            for copy in load_weights(c + 1):
                copy.start()

        for copy in load_weights(c):
            copy.wait()
        matmul_block((wk_out, wv_out), [block.at[i] for i in range(parts)], stage, c)

    for i, copy in enumerate(to_theirs + to_slots):
        copy.wait_send()
        if i >= parts:
            copy.wait_recv()


def stage_shape(weights, seqs, group):
    layers, hk, _ = weights[0].shape
    return jax.ShapeDtypeStruct((layers // LAYERS, len(weights), LAYERS, seqs, hk, group), weights[0].dtype)


def prepare(x, scale, weights, y):
    batch, half, d = x.shape
    n_slots = batch // PIECE // 2
    parts = 2
    theirs = jax.ShapeDtypeStruct((PIECE, half, d), x.dtype)
    slot = jax.ShapeDtypeStruct((PIECE, 2 * half, d), x.dtype)
    out_shape = (theirs,) * n_slots + (slot,) * n_slots
    out_shape += tuple(jax.ShapeDtypeStruct(w.shape, w.dtype) for w in weights)
    out_shape += (stage_shape(weights, PIECE * parts, 2 * half),)
    outs = pl.pallas_call(
        functools.partial(second_kernel, n_slots),
        out_shape=out_shape,
        in_specs=[ANY] * 4 + [VMEM],
        out_specs=(VMEM,) * len(out_shape),
        scratch_shapes=[
            pltpu.VMEM((n_slots, PIECE, half, d), x.dtype),
            pltpu.VMEM((parts, PIECE, 2 * half, d), x.dtype),
            pltpu.VMEM(scale.shape, scale.dtype),
            pltpu.SemaphoreType.DMA((n_slots,)),
            pltpu.SemaphoreType.DMA,
            pltpu.SemaphoreType.DMA((2, weights[0].shape[0] // LAYERS)),
            pltpu.SemaphoreType.DMA((2 * n_slots,)),
            pltpu.SemaphoreType.DMA((2 * n_slots,)),
        ],
        compiler_params=pltpu.CompilerParams(vmem_limit_bytes=9 * 2**20, collective_id=0, has_side_effects=True),
        cost_estimate=pl.CostEstimate(flops=64 * x.size, bytes_accessed=4 * x.size, transcendentals=0),
        name="prep2",
    )(in_hbm(x), in_hbm(scale), *map(in_hbm, weights), y)
    return outs[:n_slots], outs[n_slots:2 * n_slots], outs[2 * n_slots:-1], outs[-1]


def project_kernel(plan, sources, n_pieces, carried, n_alias, keep, keep_joined, *refs):
    w_refs, refs = refs[:2], refs[2:]
    pieces, refs = refs[:n_pieces], refs[n_pieces:]
    before, refs = refs[0], refs[1 + n_alias:]
    n_joins = sum(len(source) > 1 for source in sources)
    outs, refs = refs[:2], refs[2:]
    refs, (sem, before_sem) = refs[:-2], refs[-2:]
    stage, *joined = refs if keep or not (keep_joined and n_joins) else refs[-1:] + refs[:-1]
    joined = iter(joined)
    chunks, _, per = stage.shape[:3]
    entry, old_chunks = carried
    late = [copy for c in old_chunks for copy in output_copies(outs, before, before_sem, entry, c, per)]
    for copy in late:
        copy.start()
    put = lambda i, c: output_copies(outs, stage, sem, plan[i], c, per)
    tokens = []
    for source in sources:
        if len(source) > 1:
            mine, first, theirs = source
            tokens.append(next(joined))
            join(tokens[-1], pieces[mine], first, pieces[theirs])
        else:
            tokens.append(pieces[source[0]])
    used = 0
    for i, block in enumerate(plan):
        mine = tokens[used:used + len(block)]
        used += len(block)
        last = i == len(plan) - 1 and keep

        @pl.loop(0, chunks)
        def _(c):
            if i > 0:
                for copy in put(i - 1, c):
                    copy.wait()
            matmul_block(w_refs, mine, stage, c)
            if last:

                @pl.when(c < chunks - 1)
                def _():
                    for copy in put(i, c):
                        copy.start()
            else:
                for copy in put(i, c):
                    copy.start()

    for copy in late:
        copy.wait()
    for c in range(chunks - 1 if keep else chunks):
        for copy in put(len(plan) - 1, c):
            copy.wait()


def project(weights, blocks, out, carry, batch, tp, keep, keep_joined):
    layers, hk, d = weights[0].shape
    pieces, sources, joined, plan = [], [], (), []
    for block in blocks:
        entry = []
        for piece, *where in block:
            if isinstance(piece, tuple):
                mine, first, theirs = piece
                sources.append((len(pieces), first, len(pieces) + 1))
                pieces += [mine, theirs]
                n, half, _ = theirs.shape
                joined += (jax.ShapeDtypeStruct((n, 2 * half, d), theirs.dtype),)
                group = 2 * half
            else:
                sources.append((len(pieces),))
                pieces.append(piece)
                n, group, _ = piece.shape
            entry.append((n, *where))
        plan.append(tuple(entry))
    plan = tuple(plan)
    shape = jax.ShapeDtypeStruct((layers, batch, hk, group * tp // 2), weights[0].dtype)
    n_alias = 0 if out is None else 2
    n_in = 3 + len(pieces)
    stage = stage_shape(weights, sum(n for n, *_ in plan[0]), group)
    before, before_entry, chunks = carry
    tok = sum(n for entry in plan for n, *_ in entry) * group
    outs = pl.pallas_call(
        functools.partial(project_kernel, plan, tuple(sources), len(pieces), (before_entry, chunks), n_alias, keep, keep_joined),
        out_shape=(shape, shape) + (stage,) * keep + joined * keep_joined,
        in_specs=[VMEM] * n_in + [ANY] * n_alias,
        out_specs=(ANY, ANY) + (VMEM,) * (keep + len(joined) * keep_joined),
        input_output_aliases={n_in + i: i for i in range(n_alias)},
        scratch_shapes=[pltpu.VMEM(stage.shape, stage.dtype)] * (not keep) + [pltpu.VMEM(j.shape, j.dtype) for j in joined * (not keep_joined)] + [
            pltpu.SemaphoreType.DMA((stage.shape[0], 2, len(plan[0]))),
            pltpu.SemaphoreType.DMA((stage.shape[0], 2, len(before_entry))),
        ],
        compiler_params=pltpu.CompilerParams(vmem_limit_bytes=5 * 2**20),
        cost_estimate=pl.CostEstimate(
            flops=2 * tok * d * hk * 2 * layers,
            bytes_accessed=2 * tok * (d + 2 * layers * hk),
            transcendentals=0,
        ),
    )(*weights, *pieces, before, *(out or ()))
    carry = (outs[2], plan[-1], (stage.shape[0] - 1,)) if keep else None
    return outs[:2], carry, outs[2 + keep:]


def solution(mesh):
    tp = mesh.shape["tp"]
    chips = tp // 2
    ring = [(i, (i + 2 - 4 * (i % 2)) % tp) for i in range(tp)]
    swap = [(i, i ^ 1) for i in range(tp)]

    def send(v, perm):
        return lax.ppermute(v, "tp", perm)

    def per_device(enc_out, norm_scale, w_key, w_value):
        layers, d, heads, k = w_key.shape
        batch = enc_out.shape[0]
        wk = w_key.reshape(layers, d, heads * k).transpose(0, 2, 1)
        wv = w_value.reshape(layers, d, heads * k).transpose(0, 2, 1)
        n = batch // PIECE
        h = n // 2
        seq = lambda i: (i % n) * PIECE

        state = {"out": None}

        def run(blocks, keep=True, keep_joined=True):
            state["out"], state["carry"], joined = project(weights, blocks, state["out"], state["carry"], batch, tp, keep, keep_joined)
            return joined

        def hold(*arrays):
            arrays, state["out"] = lax.optimization_barrier((arrays, state["out"]))
            return arrays if len(arrays) > 1 else arrays[0]

        y = normalize_first(enc_out, norm_scale)
        ny = send(y, ring)
        other, slots, weights, stage = prepare(enc_out, norm_scale, (wk, wv), y)
        own = lambda i: ((0, seq(i)), (0, seq(i + h)))
        state["carry"] = (stage, tuple((PIECE, *own(i)) for i in range(2)), tuple(range(stage.shape[0])))
        nz = [send(v, ring) for v in other]
        n3 = send(slots[0], ring)
        run([[((y, 2 * PIECE, other[2]), *own(2)), (slots[0], *own(3))]], keep_joined=False)
        run([[(slots[1], *own(4)), (slots[2], *own(5))]])

        LEFT, RIGHT = chips - 1, 1
        near = lambda i: ((LEFT, seq(i)), (RIGHT, seq(i + h)))
        far = lambda i: ((2, seq(i)), (2, seq(i + h)))
        mine = lambda p, where: (p, *where)
        theirs = lambda q, where: (q, *where[::-1])

        py, z0, z1 = hold(ny, nz[0], nz[1])
        n4, n5 = send(slots[1], ring), send(slots[2], ring)
        p0, p1 = run([[mine((py, 0, z0), near(0)), mine((py, PIECE, z1), near(1))]])
        q0, q1 = send(p0, swap), send(p1, swap)
        z2 = hold(nz[2])
        p2, = run([[mine((py, 2 * PIECE, z2), near(2))]])
        q2 = send(p2, swap)
        run([[theirs(q0, near(0)), theirs(q1, near(1))]])
        p3 = hold(n3)
        q3 = send(p3, swap)
        run([[theirs(q2, near(2)), mine(p3, near(3))]])
        p4, p0, p1, p2 = hold(n4, p0, p1, p2)
        q4 = send(p4, swap)
        f0, f1, f2 = (send(p, ring) for p in (p0, p1, p2))
        run([[theirs(q3, near(3)), mine(p4, near(4))]])
        p5 = hold(n5)
        q5 = send(p5, swap)
        run([[theirs(q4, near(4)), mine(p5, near(5))]])
        run([[theirs(q5, near(5))]])
        for i, v in enumerate((f0, f1, f2)):
            p = hold(v)
            q = send(p, swap)
            run([[mine(p, far(i))]])
            q = hold(q)
            run([[theirs(q, far(i))]], keep=i < 2)
        out = state["out"]
        to_cache = lambda o: o.reshape(layers, batch, heads, k, -1).transpose(0, 1, 4, 2, 3)
        return to_cache(out[0]), to_cache(out[1])

    weight_spec = P(None, None, "tp", None)
    cache_spec = P(None, "dp", None, "tp", None)
    step = jax.shard_map(per_device, mesh=mesh, in_specs=(P("dp", "tp", None), P(None), weight_spec, weight_spec), out_specs=(cache_spec, cache_spec), check_vma=False)

    def program(*args):
        jax.eval_shape(step, *args)
        return step(*args)

    return program
```

```python
import functools

import jax
import jax.numpy as jnp
from jax import lax
from jax.experimental import pallas as pl
from jax.experimental.pallas import tpu as pltpu
from jax.sharding import PartitionSpec as P


NORM_EPS = 1e-6
PIECE = 2
LAYERS = 2
ANY = pl.BlockSpec(memory_space=pl.ANY)
VMEM = pl.BlockSpec(memory_space=pltpu.VMEM)
NT = (((1,), (1,)), ((), ()))
MESH = pl.DeviceIdType.MESH


def in_hbm(x):
    return pltpu.with_memory_space_constraint(x, pltpu.HBM)


def rms_norm(x, scale):
    acts = x.astype(jnp.float32)
    mean_sq = jnp.mean(acts * acts, axis=-1, keepdims=True)
    return (acts * lax.rsqrt(mean_sq + NORM_EPS) * scale).astype(jnp.bfloat16)


def output_copies(outs, stage, sem, entry, c, per):
    chips = lax.axis_size("tp") // 2
    me = lax.axis_index("tp")
    core, chip = lax.rem(me, 2), me // 2
    group = stage.shape[-1]
    copies = []
    at = 0
    for j, (n, on0, on1) in enumerate(entry):
        off, first = (a if a is b else jnp.where(core == 0, a, b) for a, b in zip(on0, on1))
        lanes = pl.ds(pl.multiple_of(lax.rem(chip + off, chips) * group, group), group)
        for kv, out in enumerate(outs):
            dst = out.at[pl.ds(c * per, per), pl.ds(first, n), :, lanes]
            copies.append(pltpu.make_async_copy(stage.at[c, kv, :, pl.ds(at, n)], dst, sem.at[c, kv, j]))
        at += n
    return copies


def matmul_block(w_refs, pieces, stage, c):
    per, _, hk, group = stage.shape[2:]
    d = w_refs[0].shape[-1]
    tokens = [p[...].reshape(-1, d) for p in pieces]
    y = jnp.concatenate(tokens) if len(tokens) > 1 else tokens[0]
    for kv, w_ref in enumerate(w_refs):
        w = w_ref[pl.ds(c * per, per)].reshape(per * hk, d)
        res = lax.dot_general(w, y, NT, preferred_element_type=jnp.float32).astype(stage.dtype)
        for l in range(per):
            for s in range(y.shape[0] // group):
                stage[c, kv, l, s] = res[l * hk:(l + 1) * hk, s * group:(s + 1) * group]


def first_kernel(x_ref, scale_ref, y_ref, xbuf, scale_buf, sem, scale_sem):
    n = y_ref.shape[0]
    start = lax.rem(lax.axis_index("tp"), 2) * n
    load = lambda i: pltpu.make_async_copy(x_ref.at[pl.ds(start + i, 1)], xbuf.at[pl.ds(i, 1)], sem.at[i])
    get_scale = pltpu.make_async_copy(scale_ref, scale_buf, scale_sem)
    get_scale.start()
    for i in range(n):
        load(i).start()
    get_scale.wait()
    scale = scale_buf[...].astype(jnp.float32).reshape(1, -1)
    for i in range(n):
        load(i).wait()
        y_ref[i] = rms_norm(xbuf[i], scale)


def normalize_first(x, scale):
    batch, half, d = x.shape
    n = batch // 2
    return pl.pallas_call(
        first_kernel,
        out_shape=jax.ShapeDtypeStruct((n, half, d), x.dtype),
        in_specs=[ANY, ANY],
        out_specs=VMEM,
        scratch_shapes=[
            pltpu.VMEM((n, half, d), x.dtype),
            pltpu.VMEM(scale.shape, scale.dtype),
            pltpu.SemaphoreType.DMA((n,)),
            pltpu.SemaphoreType.DMA,
        ],
        compiler_params=pltpu.CompilerParams(vmem_limit_bytes=8 * 2**20),
        cost_estimate=pl.CostEstimate(flops=32 * x.size, bytes_accessed=2 * x.size, transcendentals=0),
        name="first",
    )(in_hbm(x), in_hbm(scale))


def join(joined, mine, theirs, first, at):
    n, half = joined.shape[0], theirs.shape[1]
    core = lax.rem(lax.axis_index("tp"), 2)
    for s in range(n):
        joined[s, pl.ds(pl.multiple_of(core * half, half), half)] = mine[first + s]
        joined[s, pl.ds(pl.multiple_of((1 - core) * half, half), half)] = theirs[at + s]


def second_kernel(n_slots, x_ref, scale_ref, wk_ref, wv_ref, y_ref, *refs):
    theirs, refs = refs[:2], refs[2:]
    slots, refs = refs[:n_slots], refs[n_slots:]
    wk_out, wv_out, stage, xbuf, block, scale_buf, in_sem, scale_sem, w_sem, send_sem, recv_sem = refs
    half = x_ref.shape[1]
    me = lax.axis_index("tp")
    core = lax.rem(me, 2)
    other = me + 1 - 2 * core
    rows = pl.ds(pl.multiple_of(core * half, half), half)
    start = (1 - core) * n_slots * PIECE

    barrier = pltpu.get_barrier_semaphore()
    pl.semaphore_signal(barrier, inc=1, device_id={"tp": other}, device_id_type=MESH)

    def load(i):
        return pltpu.make_async_copy(x_ref.at[pl.ds(start + i * PIECE, PIECE)], xbuf.at[i], in_sem.at[i])

    def send(i, src, dst):
        return pltpu.make_async_remote_copy(
            src_ref=src,
            dst_ref=dst,
            send_sem=send_sem.at[i],
            recv_sem=recv_sem.at[i],
            device_id={"tp": other},
            device_id_type=MESH,
        )

    def load_weights(c):
        layers = pl.ds(c * LAYERS, LAYERS)
        pairs = ((wk_ref, wk_out), (wv_ref, wv_out))
        return [pltpu.make_async_copy(a.at[layers], b.at[layers], w_sem.at[kv, c]) for kv, (a, b) in enumerate(pairs)]

    get_scale = pltpu.make_async_copy(scale_ref, scale_buf, scale_sem)
    get_scale.start()
    for i in range(n_slots):
        load(i).start()
    for copy in load_weights(0):
        copy.start()
    parts = block.shape[0]
    to_theirs = [send(i, xbuf.at[i], theirs[i // parts].at[pl.ds(i % parts * PIECE, PIECE)]) for i in range(n_slots)]
    to_slots = [send(n_slots + i, y_ref.at[pl.ds(i * PIECE, PIECE)], slots[i].at[:, rows]) for i in range(n_slots)]
    get_scale.wait()
    scale = scale_buf[...].astype(jnp.float32).reshape(1, -1)
    pl.semaphore_wait(barrier, 1)
    for i in range(n_slots):
        load(i).wait()
        y = rms_norm(xbuf[i], scale)
        xbuf[i] = y
        slots[i][:, rows] = y
        if i > 0:
            to_theirs[i - 1].start()
    for copy in to_slots:
        copy.start()
    to_theirs[-1].start()
    for i in range(parts):
        to_theirs[i].wait_recv()
        join(block.at[i], y_ref, theirs[0], i * PIECE, i * PIECE)
    chunks = stage.shape[0]

    @pl.loop(0, chunks)
    def _(c):

        @pl.when(c + 1 < chunks)
        def _():
            for copy in load_weights(c + 1):
                copy.start()

        for copy in load_weights(c):
            copy.wait()
        matmul_block((wk_out, wv_out), [block.at[i] for i in range(parts)], stage, c)

    for i, copy in enumerate(to_theirs + to_slots):
        copy.wait_send()
        if i >= parts:
            copy.wait_recv()


def stage_shape(weights, seqs, group):
    layers, hk, _ = weights[0].shape
    return jax.ShapeDtypeStruct((layers // LAYERS, len(weights), LAYERS, seqs, hk, group), weights[0].dtype)


def prepare(x, scale, weights, y):
    batch, half, d = x.shape
    n_slots = batch // PIECE // 2
    parts = 2
    theirs = tuple(jax.ShapeDtypeStruct((n * PIECE, half, d), x.dtype) for n in (parts, n_slots - parts))
    slot = jax.ShapeDtypeStruct((PIECE, 2 * half, d), x.dtype)
    out_shape = theirs + (slot,) * n_slots
    out_shape += tuple(jax.ShapeDtypeStruct(w.shape, w.dtype) for w in weights)
    out_shape += (stage_shape(weights, PIECE * parts, 2 * half),)
    outs = pl.pallas_call(
        functools.partial(second_kernel, n_slots),
        out_shape=out_shape,
        in_specs=[ANY] * 4 + [VMEM],
        out_specs=(VMEM,) * len(out_shape),
        scratch_shapes=[
            pltpu.VMEM((n_slots, PIECE, half, d), x.dtype),
            pltpu.VMEM((parts, PIECE, 2 * half, d), x.dtype),
            pltpu.VMEM(scale.shape, scale.dtype),
            pltpu.SemaphoreType.DMA((n_slots,)),
            pltpu.SemaphoreType.DMA,
            pltpu.SemaphoreType.DMA((2, weights[0].shape[0] // LAYERS)),
            pltpu.SemaphoreType.DMA((2 * n_slots,)),
            pltpu.SemaphoreType.DMA((2 * n_slots,)),
        ],
        compiler_params=pltpu.CompilerParams(vmem_limit_bytes=9 * 2**20, collective_id=0, has_side_effects=True),
        cost_estimate=pl.CostEstimate(flops=64 * x.size, bytes_accessed=4 * x.size, transcendentals=0),
        name="prep2",
    )(in_hbm(x), in_hbm(scale), *map(in_hbm, weights), y)
    return outs[:2], outs[2:2 + n_slots], outs[2 + n_slots:-1], outs[-1]


def project_kernel(plan, sources, n_pieces, carried, n_alias, keep, keep_joined, unroll, *refs):
    w_refs, refs = refs[:2], refs[2:]
    pieces, refs = refs[:n_pieces], refs[n_pieces:]
    before, refs = refs[0], refs[1 + n_alias:]
    n_joins = sum(len(source) > 1 for source in sources)
    outs, refs = refs[:2], refs[2:]
    refs, (sem, before_sem) = refs[:-2], refs[-2:]
    stage, *joined = refs if keep or not (keep_joined and n_joins) else refs[-1:] + refs[:-1]
    joined = iter(joined)
    chunks, _, per = stage.shape[:3]
    entry, old_chunks = carried
    late = [copy for c in old_chunks for copy in output_copies(outs, before, before_sem, entry, c, per)]
    for copy in late:
        copy.start()
    put = lambda i, c: output_copies(outs, stage, sem, plan[i], c, per)
    tokens = []
    for source in sources:
        if len(source) > 1:
            mine, theirs, first, at = source
            tokens.append(next(joined))
            join(tokens[-1], pieces[mine], pieces[theirs], first, at)
        else:
            tokens.append(pieces[source[0]])
    used = 0
    for i, block in enumerate(plan):
        mine = tokens[used:used + len(block)]
        used += len(block)
        last = i == len(plan) - 1 and keep
        if unroll:
            for c in range(chunks):
                matmul_block(w_refs, mine, stage, c)
                if not keep and c >= chunks - 2:
                    for copy in [copy for done in (range(c + 1) if c == chunks - 2 else [c]) for copy in put(i, done)]:
                        copy.start()
            continue

        @pl.loop(0, chunks)
        def _(c):
            if i > 0:
                for copy in put(i - 1, c):
                    copy.wait()
            matmul_block(w_refs, mine, stage, c)
            if last:

                @pl.when(c < chunks - 1)
                def _():
                    for copy in put(i, c):
                        copy.start()
            else:
                for copy in put(i, c):
                    copy.start()

    for copy in late:
        copy.wait()
    for c in range((0 if unroll else chunks - 1) if keep else chunks):
        for copy in put(len(plan) - 1, c):
            copy.wait()


def project(weights, blocks, out, carry, batch, tp, keep, keep_joined, unroll):
    layers, hk, d = weights[0].shape
    pieces, sources, joined, plan = [], [], (), []
    for block in blocks:
        entry = []
        for piece, *where in block:
            if isinstance(piece, tuple):
                mine, theirs, first, at = piece
                sources.append((len(pieces), len(pieces) + 1, first, at))
                pieces += [mine, theirs]
                n, half = PIECE, theirs.shape[1]
                joined += (jax.ShapeDtypeStruct((n, 2 * half, d), theirs.dtype),)
                group = 2 * half
            else:
                sources.append((len(pieces),))
                pieces.append(piece)
                n, group, _ = piece.shape
            entry.append((n, *where))
        plan.append(tuple(entry))
    plan = tuple(plan)
    shape = jax.ShapeDtypeStruct((layers, batch, hk, group * tp // 2), weights[0].dtype)
    n_alias = 0 if out is None else 2
    n_in = 3 + len(pieces)
    stage = stage_shape(weights, sum(n for n, *_ in plan[0]), group)
    before, before_entry, chunks = carry
    tok = sum(n for entry in plan for n, *_ in entry) * group
    outs = pl.pallas_call(
        functools.partial(project_kernel, plan, tuple(sources), len(pieces), (before_entry, chunks), n_alias, keep, keep_joined, unroll),
        out_shape=(shape, shape) + (stage,) * keep + joined * keep_joined,
        in_specs=[VMEM] * n_in + [ANY] * n_alias,
        out_specs=(ANY, ANY) + (VMEM,) * (keep + len(joined) * keep_joined),
        input_output_aliases={n_in + i: i for i in range(n_alias)},
        scratch_shapes=[pltpu.VMEM(stage.shape, stage.dtype)] * (not keep) + [pltpu.VMEM(j.shape, j.dtype) for j in joined * (not keep_joined)] + [
            pltpu.SemaphoreType.DMA((stage.shape[0], 2, len(plan[0]))),
            pltpu.SemaphoreType.DMA((stage.shape[0], 2, len(before_entry))),
        ],
        compiler_params=pltpu.CompilerParams(vmem_limit_bytes=5 * 2**20),
        cost_estimate=pl.CostEstimate(
            flops=2 * tok * d * hk * 2 * layers,
            bytes_accessed=2 * tok * (d + 2 * layers * hk),
            transcendentals=0,
        ),
    )(*weights, *pieces, before, *(out or ()))
    chunks = stage.shape[0]
    carry = (outs[2], plan[-1], tuple(range(0 if unroll else chunks - 1, chunks))) if keep else None
    return outs[:2], carry, outs[2 + keep:]


def solution(mesh):
    tp = mesh.shape["tp"]
    chips = tp // 2
    ring = [(i, (i + 2 - 4 * (i % 2)) % tp) for i in range(tp)]
    swap = [(i, i ^ 1) for i in range(tp)]

    def send(v, perm):
        return lax.ppermute(v, "tp", perm)

    def per_device(enc_out, norm_scale, w_key, w_value):
        layers, d, heads, k = w_key.shape
        batch = enc_out.shape[0]
        wk = w_key.reshape(layers, d, heads * k).transpose(0, 2, 1)
        wv = w_value.reshape(layers, d, heads * k).transpose(0, 2, 1)
        n = batch // PIECE
        h = n // 2
        seq = lambda i: (i % n) * PIECE

        state = {"out": None}

        def run(blocks, keep=True, keep_joined=True, unroll=False):
            state["out"], state["carry"], joined = project(weights, blocks, state["out"], state["carry"], batch, tp, keep, keep_joined, unroll)
            return joined

        def hold(*arrays):
            arrays, state["out"] = lax.optimization_barrier((arrays, state["out"]))
            return arrays if len(arrays) > 1 else arrays[0]

        y = normalize_first(enc_out, norm_scale)
        ny = send(y, ring)
        other, slots, weights, stage = prepare(enc_out, norm_scale, (wk, wv), y)
        own = lambda i: ((0, seq(i)), (0, seq(i + h)))
        state["carry"] = (stage, tuple((PIECE, *own(i)) for i in range(2)), tuple(range(stage.shape[0])))
        nz = [send(v, ring) for v in other]
        n3 = send(slots[0], ring)
        run([[((y, other[1], 2 * PIECE, 0), *own(2)), (slots[0], *own(3))]], keep_joined=False)
        run([[(slots[1], *own(4)), (slots[2], *own(5))]])

        LEFT, RIGHT = chips - 1, 1
        near = lambda i: ((LEFT, seq(i)), (RIGHT, seq(i + h)))
        far = lambda i: ((2, seq(i)), (2, seq(i + h)))
        mine = lambda p, where: (p, *where)
        theirs = lambda q, where: (q, *where[::-1])

        py, z0 = hold(ny, nz[0])
        n4, n5 = send(slots[1], ring), send(slots[2], ring)
        p0, p1 = run([[mine((py, z0, 0, 0), near(0)), mine((py, z0, PIECE, PIECE), near(1))]])
        q0, q1 = send(p0, swap), send(p1, swap)
        z1 = hold(nz[1])
        p2, = run([[mine((py, z1, 2 * PIECE, 0), near(2))]])
        q2 = send(p2, swap)
        run([[theirs(q0, near(0)), theirs(q1, near(1))]])
        p3 = hold(n3)
        q3 = send(p3, swap)
        run([[theirs(q2, near(2)), mine(p3, near(3))]])
        p4, p0, p1, p2 = hold(n4, p0, p1, p2)
        q4 = send(p4, swap)
        f0, f1, f2 = (send(p, ring) for p in (p0, p1, p2))
        run([[theirs(q3, near(3)), mine(p4, near(4))]])
        p5 = hold(n5)
        q5 = send(p5, swap)
        run([[theirs(q4, near(4)), mine(p5, near(5))]])
        run([[theirs(q5, near(5))]])
        for i, v in enumerate((f0, f1, f2)):
            p = hold(v)
            q = send(p, swap)
            run([[mine(p, far(i))]], unroll=i == 2)
            q = hold(q)
            run([[theirs(q, far(i))]], keep=i < 2, unroll=i == 2)
        out = state["out"]
        to_cache = lambda o: o.reshape(layers, batch, heads, k, -1).transpose(0, 1, 4, 2, 3)
        return to_cache(out[0]), to_cache(out[1])

    weight_spec = P(None, None, "tp", None)
    cache_spec = P(None, "dp", None, "tp", None)
    step = jax.shard_map(per_device, mesh=mesh, in_specs=(P("dp", "tp", None), P(None), weight_spec, weight_spec), out_specs=(cache_spec, cache_spec), check_vma=False)

    def program(*args):
        jax.eval_shape(step, *args)
        return step(*args)

    return program
```

```python
import functools

import jax
import jax.numpy as jnp
from jax import lax
from jax.experimental import pallas as pl
from jax.experimental.pallas import tpu as pltpu
from jax.sharding import PartitionSpec as P


NORM_EPS = 1e-6
PIECE = 2
LAYERS = 2
ANY = pl.BlockSpec(memory_space=pl.ANY)
VMEM = pl.BlockSpec(memory_space=pltpu.VMEM)
NT = (((1,), (1,)), ((), ()))
MESH = pl.DeviceIdType.MESH


def in_hbm(x):
    return pltpu.with_memory_space_constraint(x, pltpu.HBM)


def rms_norm(x, scale):
    acts = x.astype(jnp.float32)
    mean_sq = jnp.mean(acts * acts, axis=-1, keepdims=True)
    return (acts * lax.rsqrt(mean_sq + NORM_EPS) * scale).astype(jnp.bfloat16)


def output_copies(outs, stage, sem, entry, c, per):
    chips = lax.axis_size("tp") // 2
    me = lax.axis_index("tp")
    core, chip = lax.rem(me, 2), me // 2
    group = stage.shape[-1]
    copies = []
    at = 0
    for j, (n, on0, on1) in enumerate(entry):
        off, first = (a if a is b else jnp.where(core == 0, a, b) for a, b in zip(on0, on1))
        lanes = pl.ds(pl.multiple_of(lax.rem(chip + off, chips) * group, group), group)
        for kv, out in enumerate(outs):
            dst = out.at[pl.ds(c * per, per), pl.ds(first, n), :, lanes]
            copies.append(pltpu.make_async_copy(stage.at[c, kv, :, pl.ds(at, n)], dst, sem.at[c, kv, j]))
        at += n
    return copies


def matmul_block(w_refs, pieces, stage, c):
    per, _, hk, group = stage.shape[2:]
    d = w_refs[0].shape[-1]
    tokens = [p[...].reshape(-1, d) for p in pieces]
    y = jnp.concatenate(tokens) if len(tokens) > 1 else tokens[0]
    for kv, w_ref in enumerate(w_refs):
        w = w_ref[pl.ds(c * per, per)].reshape(per * hk, d)
        res = lax.dot_general(w, y, NT, preferred_element_type=jnp.float32).astype(stage.dtype)
        for l in range(per):
            for s in range(y.shape[0] // group):
                stage[c, kv, l, s] = res[l * hk:(l + 1) * hk, s * group:(s + 1) * group]


def first_kernel(skip, x_ref, scale_ref, y_ref, xbuf, scale_buf, sem, scale_sem):
    n = y_ref.shape[0]
    start = lax.rem(lax.axis_index("tp"), 2) * (x_ref.shape[0] // 2) + skip
    load = lambda i: pltpu.make_async_copy(x_ref.at[pl.ds(start + i, 1)], xbuf.at[pl.ds(i, 1)], sem.at[i])
    get_scale = pltpu.make_async_copy(scale_ref, scale_buf, scale_sem)
    get_scale.start()
    for i in range(n):
        load(i).start()
    get_scale.wait()
    scale = scale_buf[...].astype(jnp.float32).reshape(1, -1)
    for i in range(n):
        load(i).wait()
        y_ref[i] = rms_norm(xbuf[i], scale)


def normalize_first(x, scale, skip, n):
    _, half, d = x.shape
    return pl.pallas_call(
        functools.partial(first_kernel, skip),
        out_shape=jax.ShapeDtypeStruct((n, half, d), x.dtype),
        in_specs=[ANY, ANY],
        out_specs=VMEM,
        scratch_shapes=[
            pltpu.VMEM((n, half, d), x.dtype),
            pltpu.VMEM(scale.shape, scale.dtype),
            pltpu.SemaphoreType.DMA((n,)),
            pltpu.SemaphoreType.DMA,
        ],
        compiler_params=pltpu.CompilerParams(vmem_limit_bytes=8 * 2**20),
        cost_estimate=pl.CostEstimate(flops=32 * x.size, bytes_accessed=2 * x.size, transcendentals=0),
    )(in_hbm(x), in_hbm(scale))


def join(joined, mine, theirs, first, at):
    n, half = joined.shape[0], theirs.shape[1]
    core = lax.rem(lax.axis_index("tp"), 2)
    for s in range(n):
        joined[s, pl.ds(pl.multiple_of(core * half, half), half)] = mine[first + s]
        joined[s, pl.ds(pl.multiple_of((1 - core) * half, half), half)] = theirs[at + s]


def second_kernel(n_slots, x_ref, scale_ref, wk_ref, wv_ref, y_first, y_rest, *refs):
    theirs, refs = refs[:2], refs[2:]
    slots, refs = refs[:n_slots], refs[n_slots:]
    wk_out, wv_out, stage, xbuf, block, scale_buf, in_sem, scale_sem, w_sem, send_sem, recv_sem = refs
    half = x_ref.shape[1]
    me = lax.axis_index("tp")
    core = lax.rem(me, 2)
    other = me + 1 - 2 * core
    rows = pl.ds(pl.multiple_of(core * half, half), half)
    start = (1 - core) * n_slots * PIECE

    barrier = pltpu.get_barrier_semaphore()
    pl.semaphore_signal(barrier, inc=1, device_id={"tp": other}, device_id_type=MESH)

    def load(i):
        return pltpu.make_async_copy(x_ref.at[pl.ds(start + i * PIECE, PIECE)], xbuf.at[i], in_sem.at[i])

    def send(i, src, dst):
        return pltpu.make_async_remote_copy(
            src_ref=src,
            dst_ref=dst,
            send_sem=send_sem.at[i],
            recv_sem=recv_sem.at[i],
            device_id={"tp": other},
            device_id_type=MESH,
        )

    def load_weights(c):
        layers = pl.ds(c * LAYERS, LAYERS)
        pairs = ((wk_ref, wk_out), (wv_ref, wv_out))
        return [pltpu.make_async_copy(a.at[layers], b.at[layers], w_sem.at[kv, c]) for kv, (a, b) in enumerate(pairs)]

    get_scale = pltpu.make_async_copy(scale_ref, scale_buf, scale_sem)
    get_scale.start()
    for i in range(n_slots):
        load(i).start()
    for copy in load_weights(0):
        copy.start()
    parts = block.shape[0]
    to_theirs = [send(i, xbuf.at[i], theirs[i // parts].at[pl.ds(i % parts * PIECE, PIECE)]) for i in range(n_slots)]
    made = [y_first] + [y_rest.at[pl.ds(i * PIECE, PIECE)] for i in range(n_slots - 1)]
    to_slots = [send(n_slots + i, made[i], slots[i].at[:, rows]) for i in range(n_slots)]
    get_scale.wait()
    scale = scale_buf[...].astype(jnp.float32).reshape(1, -1)
    pl.semaphore_wait(barrier, 1)
    for i in range(n_slots):
        load(i).wait()
        y = rms_norm(xbuf[i], scale)
        xbuf[i] = y
        slots[i][:, rows] = y
        if i > 0:
            to_theirs[i - 1].start()
    for copy in to_slots:
        copy.start()
    to_theirs[-1].start()
    for i in range(parts):
        to_theirs[i].wait_recv()
        join(block.at[i], made[i], theirs[0], 0, i * PIECE)
    chunks = stage.shape[0]

    @pl.loop(0, chunks)
    def _(c):

        @pl.when(c + 1 < chunks)
        def _():
            for copy in load_weights(c + 1):
                copy.start()

        for copy in load_weights(c):
            copy.wait()
        matmul_block((wk_out, wv_out), [block.at[i] for i in range(parts)], stage, c)

    for i, copy in enumerate(to_theirs + to_slots):
        copy.wait_send()
        if i >= parts:
            copy.wait_recv()


def stage_shape(weights, seqs, group):
    layers, hk, _ = weights[0].shape
    return jax.ShapeDtypeStruct((layers // LAYERS, len(weights), LAYERS, seqs, hk, group), weights[0].dtype)


def prepare(x, scale, weights, y_first, y_rest):
    batch, half, d = x.shape
    n_slots = batch // PIECE // 2
    parts = 2
    theirs = tuple(jax.ShapeDtypeStruct((n * PIECE, half, d), x.dtype) for n in (parts, n_slots - parts))
    slot = jax.ShapeDtypeStruct((PIECE, 2 * half, d), x.dtype)
    out_shape = theirs + (slot,) * n_slots
    out_shape += tuple(jax.ShapeDtypeStruct(w.shape, w.dtype) for w in weights)
    out_shape += (stage_shape(weights, PIECE * parts, 2 * half),)
    outs = pl.pallas_call(
        functools.partial(second_kernel, n_slots),
        out_shape=out_shape,
        in_specs=[ANY] * 4 + [VMEM] * 2,
        out_specs=(VMEM,) * len(out_shape),
        scratch_shapes=[
            pltpu.VMEM((n_slots, PIECE, half, d), x.dtype),
            pltpu.VMEM((parts, PIECE, 2 * half, d), x.dtype),
            pltpu.VMEM(scale.shape, scale.dtype),
            pltpu.SemaphoreType.DMA((n_slots,)),
            pltpu.SemaphoreType.DMA,
            pltpu.SemaphoreType.DMA((2, weights[0].shape[0] // LAYERS)),
            pltpu.SemaphoreType.DMA((2 * n_slots,)),
            pltpu.SemaphoreType.DMA((2 * n_slots,)),
        ],
        compiler_params=pltpu.CompilerParams(vmem_limit_bytes=9 * 2**20, collective_id=0, has_side_effects=True),
        cost_estimate=pl.CostEstimate(flops=64 * x.size, bytes_accessed=4 * x.size, transcendentals=0),
        name="prep2",
    )(in_hbm(x), in_hbm(scale), *map(in_hbm, weights), y_first, y_rest)
    return outs[:2], outs[2:2 + n_slots], outs[2 + n_slots:-1], outs[-1]


def project_kernel(plan, sources, n_pieces, carried, n_alias, keep, keep_joined, unroll, *refs):
    w_refs, refs = refs[:2], refs[2:]
    pieces, refs = refs[:n_pieces], refs[n_pieces:]
    before, refs = refs[0], refs[1 + n_alias:]
    n_joins = sum(len(source) > 1 for source in sources)
    outs, refs = refs[:2], refs[2:]
    refs, (sem, before_sem) = refs[:-2], refs[-2:]
    stage, *joined = refs if keep or not (keep_joined and n_joins) else refs[-1:] + refs[:-1]
    joined = iter(joined)
    chunks, _, per = stage.shape[:3]
    entry, old_chunks = carried
    late = [copy for c in old_chunks for copy in output_copies(outs, before, before_sem, entry, c, per)]
    for copy in late:
        copy.start()
    put = lambda i, c: output_copies(outs, stage, sem, plan[i], c, per)
    tokens = []
    for source in sources:
        if len(source) > 1:
            mine, theirs, first, at = source
            tokens.append(next(joined))
            join(tokens[-1], pieces[mine], pieces[theirs], first, at)
        else:
            tokens.append(pieces[source[0]])
    used = 0
    for i, block in enumerate(plan):
        mine = tokens[used:used + len(block)]
        used += len(block)
        last = i == len(plan) - 1 and keep
        if unroll:
            for c in range(chunks):
                matmul_block(w_refs, mine, stage, c)
                if not keep and c >= chunks - 2:
                    for copy in [copy for done in (range(c + 1) if c == chunks - 2 else [c]) for copy in put(i, done)]:
                        copy.start()
            continue

        @pl.loop(0, chunks)
        def _(c):
            if i > 0:
                for copy in put(i - 1, c):
                    copy.wait()
            matmul_block(w_refs, mine, stage, c)
            if last:

                @pl.when(c < chunks - 1)
                def _():
                    for copy in put(i, c):
                        copy.start()
            else:
                for copy in put(i, c):
                    copy.start()

    for copy in late:
        copy.wait()
    for c in range((0 if unroll else chunks - 1) if keep else chunks):
        for copy in put(len(plan) - 1, c):
            copy.wait()


def project(weights, blocks, out, carry, batch, tp, keep, keep_joined, unroll):
    layers, hk, d = weights[0].shape
    pieces, sources, joined, plan = [], [], (), []
    for block in blocks:
        entry = []
        for piece, *where in block:
            if isinstance(piece, tuple):
                mine, theirs, first, at = piece
                sources.append((len(pieces), len(pieces) + 1, first, at))
                pieces += [mine, theirs]
                n, half = PIECE, theirs.shape[1]
                joined += (jax.ShapeDtypeStruct((n, 2 * half, d), theirs.dtype),)
                group = 2 * half
            else:
                sources.append((len(pieces),))
                pieces.append(piece)
                n, group, _ = piece.shape
            entry.append((n, *where))
        plan.append(tuple(entry))
    plan = tuple(plan)
    shape = jax.ShapeDtypeStruct((layers, batch, hk, group * tp // 2), weights[0].dtype)
    n_alias = 0 if out is None else 2
    n_in = 3 + len(pieces)
    stage = stage_shape(weights, sum(n for n, *_ in plan[0]), group)
    before, before_entry, chunks = carry
    tok = sum(n for entry in plan for n, *_ in entry) * group
    outs = pl.pallas_call(
        functools.partial(project_kernel, plan, tuple(sources), len(pieces), (before_entry, chunks), n_alias, keep, keep_joined, unroll),
        out_shape=(shape, shape) + (stage,) * keep + joined * keep_joined,
        in_specs=[VMEM] * n_in + [ANY] * n_alias,
        out_specs=(ANY, ANY) + (VMEM,) * (keep + len(joined) * keep_joined),
        input_output_aliases={n_in + i: i for i in range(n_alias)},
        scratch_shapes=[pltpu.VMEM(stage.shape, stage.dtype)] * (not keep) + [pltpu.VMEM(j.shape, j.dtype) for j in joined * (not keep_joined)] + [
            pltpu.SemaphoreType.DMA((stage.shape[0], 2, len(plan[0]))),
            pltpu.SemaphoreType.DMA((stage.shape[0], 2, len(before_entry))),
        ],
        compiler_params=pltpu.CompilerParams(vmem_limit_bytes=5 * 2**20),
        cost_estimate=pl.CostEstimate(
            flops=2 * tok * d * hk * 2 * layers,
            bytes_accessed=2 * tok * (d + 2 * layers * hk),
            transcendentals=0,
        ),
    )(*weights, *pieces, before, *(out or ()))
    chunks = stage.shape[0]
    carry = (outs[2], plan[-1], tuple(range(0 if unroll else chunks - 1, chunks))) if keep else None
    return outs[:2], carry, outs[2 + keep:]


def solution(mesh):
    tp = mesh.shape["tp"]
    chips = tp // 2
    ring = [(i, (i + 2 - 4 * (i % 2)) % tp) for i in range(tp)]
    swap = [(i, i ^ 1) for i in range(tp)]

    def send(v, perm):
        return lax.ppermute(v, "tp", perm)

    def per_device(enc_out, norm_scale, w_key, w_value):
        layers, d, heads, k = w_key.shape
        batch = enc_out.shape[0]
        wk = w_key.reshape(layers, d, heads * k).transpose(0, 2, 1)
        wv = w_value.reshape(layers, d, heads * k).transpose(0, 2, 1)
        n = batch // PIECE
        h = n // 2
        seq = lambda i: (i % n) * PIECE

        state = {"out": None}

        def run(blocks, keep=True, keep_joined=True, unroll=False):
            state["out"], state["carry"], joined = project(weights, blocks, state["out"], state["carry"], batch, tp, keep, keep_joined, unroll)
            return joined

        def hold(*arrays):
            arrays, state["out"] = lax.optimization_barrier((arrays, state["out"]))
            return arrays if len(arrays) > 1 else arrays[0]

        ya = normalize_first(enc_out, norm_scale, 0, PIECE)
        na = send(ya, ring)
        yb = normalize_first(enc_out, norm_scale, PIECE, batch // 2 - PIECE)
        nb = send(yb, ring)
        other, slots, weights, stage = prepare(enc_out, norm_scale, (wk, wv), ya, yb)
        own = lambda i: ((0, seq(i)), (0, seq(i + h)))
        state["carry"] = (stage, tuple((PIECE, *own(i)) for i in range(2)), tuple(range(stage.shape[0])))
        nz = [send(v, ring) for v in other]
        n3 = send(slots[0], ring)
        run([[((yb, other[1], PIECE, 0), *own(2)), (slots[0], *own(3))]], keep_joined=False)
        run([[(slots[1], *own(4)), (slots[2], *own(5))]])

        LEFT, RIGHT = chips - 1, 1
        near = lambda i: ((LEFT, seq(i)), (RIGHT, seq(i + h)))
        far = lambda i: ((2, seq(i)), (2, seq(i + h)))
        mine = lambda p, where: (p, *where)
        theirs = lambda q, where: (q, *where[::-1])

        pa, pb, z0 = hold(na, nb, nz[0])
        n4, n5 = send(slots[1], ring), send(slots[2], ring)
        p0, p1 = run([[mine((pa, z0, 0, 0), near(0)), mine((pb, z0, 0, PIECE), near(1))]])
        q0, q1 = send(p0, swap), send(p1, swap)
        z1 = hold(nz[1])
        p2, = run([[mine((pb, z1, PIECE, 0), near(2))]])
        q2 = send(p2, swap)
        run([[theirs(q0, near(0)), theirs(q1, near(1))]])
        p3 = hold(n3)
        q3 = send(p3, swap)
        run([[theirs(q2, near(2)), mine(p3, near(3))]])
        p4, p0, p1, p2 = hold(n4, p0, p1, p2)
        q4 = send(p4, swap)
        f0, f1, f2 = (send(p, ring) for p in (p0, p1, p2))
        run([[theirs(q3, near(3)), mine(p4, near(4))]])
        p5 = hold(n5)
        q5 = send(p5, swap)
        run([[theirs(q4, near(4)), mine(p5, near(5))]])
        run([[theirs(q5, near(5))]], unroll=True)
        for i, v in enumerate((f0, f1, f2)):
            p = hold(v)
            q = send(p, swap)
            run([[mine(p, far(i))]], unroll=i != 1)
            q = hold(q)
            run([[theirs(q, far(i))]], keep=i < 2, unroll=i == 2)
        out = state["out"]
        to_cache = lambda o: o.reshape(layers, batch, heads, k, -1).transpose(0, 1, 4, 2, 3)
        return to_cache(out[0]), to_cache(out[1])

    weight_spec = P(None, None, "tp", None)
    cache_spec = P(None, "dp", None, "tp", None)
    step = jax.shard_map(per_device, mesh=mesh, in_specs=(P("dp", "tp", None), P(None), weight_spec, weight_spec), out_specs=(cache_spec, cache_spec), check_vma=False)

    def program(*args):
        jax.eval_shape(step, *args)
        return step(*args)

    return program
```

```python
import functools

import jax
import jax.numpy as jnp
from jax import lax
from jax.experimental import pallas as pl
from jax.experimental.pallas import tpu as pltpu
from jax.sharding import PartitionSpec as P


NORM_EPS = 1e-6
PIECE = 2
LAYERS = 2
ANY = pl.BlockSpec(memory_space=pl.ANY)
VMEM = pl.BlockSpec(memory_space=pltpu.VMEM)
NT = (((1,), (1,)), ((), ()))
MESH = pl.DeviceIdType.MESH


def in_hbm(x):
    return pltpu.with_memory_space_constraint(x, pltpu.HBM)


def rms_norm(x, scale):
    acts = x.astype(jnp.float32)
    mean_sq = jnp.mean(acts * acts, axis=-1, keepdims=True)
    return (acts * lax.rsqrt(mean_sq + NORM_EPS) * scale).astype(jnp.bfloat16)


def output_copies(outs, stage, sem, entry, c, per):
    chips = lax.axis_size("tp") // 2
    me = lax.axis_index("tp")
    core, chip = lax.rem(me, 2), me // 2
    group = stage.shape[-1]
    copies = []
    at = 0
    for j, (n, on0, on1) in enumerate(entry):
        off, first = (a if a is b else jnp.where(core == 0, a, b) for a, b in zip(on0, on1))
        lanes = pl.ds(pl.multiple_of(lax.rem(chip + off, chips) * group, group), group)
        for kv, out in enumerate(outs):
            dst = out.at[pl.ds(c * per, per), pl.ds(first, n), :, lanes]
            copies.append(pltpu.make_async_copy(stage.at[c, kv, :, pl.ds(at, n)], dst, sem.at[c, kv, j]))
        at += n
    return copies


def matmul_block(w_refs, pieces, stage, c):
    per, _, hk, group = stage.shape[2:]
    d = w_refs[0].shape[-1]
    tokens = [p[...].reshape(-1, d) for p in pieces]
    y = jnp.concatenate(tokens) if len(tokens) > 1 else tokens[0]
    for kv, w_ref in enumerate(w_refs):
        w = w_ref[pl.ds(c * per, per)].reshape(per * hk, d)
        res = lax.dot_general(w, y, NT, preferred_element_type=jnp.float32).astype(stage.dtype)
        for l in range(per):
            for s in range(y.shape[0] // group):
                stage[c, kv, l, s] = res[l * hk:(l + 1) * hk, s * group:(s + 1) * group]


def first_kernel(skip, x_ref, scale_ref, y_ref, xbuf, scale_buf, sem, scale_sem):
    n = y_ref.shape[0]
    start = lax.rem(lax.axis_index("tp"), 2) * (x_ref.shape[0] // 2) + skip
    load = lambda i: pltpu.make_async_copy(x_ref.at[pl.ds(start + i, PIECE)], xbuf.at[pl.ds(i, PIECE)], sem.at[i])
    get_scale = pltpu.make_async_copy(scale_ref, scale_buf, scale_sem)
    get_scale.start()
    for i in range(0, n, PIECE):
        load(i).start()
    get_scale.wait()
    scale = scale_buf[...].astype(jnp.float32).reshape(1, -1)
    for i in range(0, n, PIECE):
        load(i).wait()
        y_ref[i:i + PIECE] = rms_norm(xbuf[i:i + PIECE], scale)


def normalize_first(x, scale, skip, n):
    _, half, d = x.shape
    return pl.pallas_call(
        functools.partial(first_kernel, skip),
        out_shape=jax.ShapeDtypeStruct((n, half, d), x.dtype),
        in_specs=[ANY, ANY],
        out_specs=VMEM,
        scratch_shapes=[
            pltpu.VMEM((n, half, d), x.dtype),
            pltpu.VMEM(scale.shape, scale.dtype),
            pltpu.SemaphoreType.DMA((n,)),
            pltpu.SemaphoreType.DMA,
        ],
        compiler_params=pltpu.CompilerParams(vmem_limit_bytes=8 * 2**20),
        cost_estimate=pl.CostEstimate(flops=32 * x.size, bytes_accessed=2 * x.size, transcendentals=0),
    )(in_hbm(x), in_hbm(scale))


def join(joined, mine, theirs, first, at):
    n, half = joined.shape[0], theirs.shape[1]
    core = lax.rem(lax.axis_index("tp"), 2)
    for s in range(n):
        joined[s, pl.ds(pl.multiple_of(core * half, half), half)] = mine[first + s]
        joined[s, pl.ds(pl.multiple_of((1 - core) * half, half), half)] = theirs[at + s]


def second_kernel(n_slots, x_ref, scale_ref, wk_ref, wv_ref, y_first, y_rest, *refs):
    theirs, refs = refs[:2], refs[2:]
    slots, refs = refs[:n_slots], refs[n_slots:]
    wk_out, wv_out, stage, xbuf, block, scale_buf, in_sem, scale_sem, w_sem, send_sem, recv_sem = refs
    half = x_ref.shape[1]
    me = lax.axis_index("tp")
    core = lax.rem(me, 2)
    other = me + 1 - 2 * core
    rows = pl.ds(pl.multiple_of(core * half, half), half)
    start = (1 - core) * n_slots * PIECE

    barrier = pltpu.get_barrier_semaphore()
    pl.semaphore_signal(barrier, inc=1, device_id={"tp": other}, device_id_type=MESH)

    def load(i):
        return pltpu.make_async_copy(x_ref.at[pl.ds(start + i * PIECE, PIECE)], xbuf.at[i], in_sem.at[i])

    def send(i, src, dst):
        return pltpu.make_async_remote_copy(
            src_ref=src,
            dst_ref=dst,
            send_sem=send_sem.at[i],
            recv_sem=recv_sem.at[i],
            device_id={"tp": other},
            device_id_type=MESH,
        )

    def load_weights(c):
        layers = pl.ds(c * LAYERS, LAYERS)
        pairs = ((wk_ref, wk_out), (wv_ref, wv_out))
        return [pltpu.make_async_copy(a.at[layers], b.at[layers], w_sem.at[kv, c]) for kv, (a, b) in enumerate(pairs)]

    get_scale = pltpu.make_async_copy(scale_ref, scale_buf, scale_sem)
    get_scale.start()
    for i in range(n_slots):
        load(i).start()
    for copy in load_weights(0):
        copy.start()
    parts = block.shape[0]
    to_theirs = [send(i, xbuf.at[i], theirs[i // parts].at[pl.ds(i % parts * PIECE, PIECE)]) for i in range(n_slots)]
    made = [y_first] + [y_rest.at[pl.ds(i * PIECE, PIECE)] for i in range(n_slots - 1)]
    to_slots = [send(n_slots + i, made[i], slots[i].at[:, rows]) for i in range(n_slots)]
    get_scale.wait()
    scale = scale_buf[...].astype(jnp.float32).reshape(1, -1)
    pl.semaphore_wait(barrier, 1)
    for i in range(n_slots):
        load(i).wait()
        y = rms_norm(xbuf[i], scale)
        xbuf[i] = y
        slots[i][:, rows] = y
        if i > 0:
            to_theirs[i - 1].start()
    for copy in to_slots:
        copy.start()
    to_theirs[-1].start()
    for i in range(parts):
        to_theirs[i].wait_recv()
        join(block.at[i], made[i], theirs[0], 0, i * PIECE)
    chunks = stage.shape[0]

    @pl.loop(0, chunks)
    def _(c):

        @pl.when(c + 1 < chunks)
        def _():
            for copy in load_weights(c + 1):
                copy.start()

        for copy in load_weights(c):
            copy.wait()
        matmul_block((wk_out, wv_out), [block.at[i] for i in range(parts)], stage, c)

    for i, copy in enumerate(to_theirs + to_slots):
        copy.wait_send()
        if i >= parts:
            copy.wait_recv()


def stage_shape(weights, seqs, group):
    layers, hk, _ = weights[0].shape
    return jax.ShapeDtypeStruct((layers // LAYERS, len(weights), LAYERS, seqs, hk, group), weights[0].dtype)


def prepare(x, scale, weights, y_first, y_rest):
    batch, half, d = x.shape
    n_slots = batch // PIECE // 2
    parts = 2
    theirs = tuple(jax.ShapeDtypeStruct((n * PIECE, half, d), x.dtype) for n in (parts, n_slots - parts))
    slot = jax.ShapeDtypeStruct((PIECE, 2 * half, d), x.dtype)
    out_shape = theirs + (slot,) * n_slots
    out_shape += tuple(jax.ShapeDtypeStruct(w.shape, w.dtype) for w in weights)
    out_shape += (stage_shape(weights, PIECE * parts, 2 * half),)
    outs = pl.pallas_call(
        functools.partial(second_kernel, n_slots),
        out_shape=out_shape,
        in_specs=[ANY] * 4 + [VMEM] * 2,
        out_specs=(VMEM,) * len(out_shape),
        scratch_shapes=[
            pltpu.VMEM((n_slots, PIECE, half, d), x.dtype),
            pltpu.VMEM((parts, PIECE, 2 * half, d), x.dtype),
            pltpu.VMEM(scale.shape, scale.dtype),
            pltpu.SemaphoreType.DMA((n_slots,)),
            pltpu.SemaphoreType.DMA,
            pltpu.SemaphoreType.DMA((2, weights[0].shape[0] // LAYERS)),
            pltpu.SemaphoreType.DMA((2 * n_slots,)),
            pltpu.SemaphoreType.DMA((2 * n_slots,)),
        ],
        compiler_params=pltpu.CompilerParams(vmem_limit_bytes=9 * 2**20, collective_id=0, has_side_effects=True),
        cost_estimate=pl.CostEstimate(flops=64 * x.size, bytes_accessed=4 * x.size, transcendentals=0),
        name="prep2",
    )(in_hbm(x), in_hbm(scale), *map(in_hbm, weights), y_first, y_rest)
    return outs[:2], outs[2:2 + n_slots], outs[2 + n_slots:-1], outs[-1]


def project_kernel(plan, sources, n_pieces, carried, n_alias, keep, keep_joined, unroll, *refs):
    w_refs, refs = refs[:2], refs[2:]
    pieces, refs = refs[:n_pieces], refs[n_pieces:]
    before, refs = refs[0], refs[1 + n_alias:]
    n_joins = sum(len(source) > 1 for source in sources)
    outs, refs = refs[:2], refs[2:]
    refs, (sem, before_sem) = refs[:-2], refs[-2:]
    stage, *joined = refs if keep or not (keep_joined and n_joins) else refs[-1:] + refs[:-1]
    joined = iter(joined)
    chunks, _, per = stage.shape[:3]
    entry, old_chunks = carried
    late = [copy for c in old_chunks for copy in output_copies(outs, before, before_sem, entry, c, per)]
    for copy in late:
        copy.start()
    put = lambda i, c: output_copies(outs, stage, sem, plan[i], c, per)
    tokens = []
    for source in sources:
        if len(source) > 1:
            mine, theirs, first, at = source
            tokens.append(next(joined))
            join(tokens[-1], pieces[mine], pieces[theirs], first, at)
        else:
            tokens.append(pieces[source[0]])
    used = 0
    for i, block in enumerate(plan):
        mine = tokens[used:used + len(block)]
        used += len(block)
        last = i == len(plan) - 1 and keep
        if unroll:
            for c in range(chunks):
                matmul_block(w_refs, mine, stage, c)
                if not keep and c >= chunks - 2:
                    for copy in [copy for done in (range(c + 1) if c == chunks - 2 else [c]) for copy in put(i, done)]:
                        copy.start()
            continue

        @pl.loop(0, chunks)
        def _(c):
            if i > 0:
                for copy in put(i - 1, c):
                    copy.wait()
            matmul_block(w_refs, mine, stage, c)
            if last:

                @pl.when(c < chunks - 1)
                def _():
                    for copy in put(i, c):
                        copy.start()
            else:
                for copy in put(i, c):
                    copy.start()

    for copy in late:
        copy.wait()
    for c in range((0 if unroll else chunks - 1) if keep else chunks):
        for copy in put(len(plan) - 1, c):
            copy.wait()


def project(weights, blocks, out, carry, batch, tp, keep, keep_joined, unroll):
    layers, hk, d = weights[0].shape
    pieces, sources, joined, plan = [], [], (), []
    for block in blocks:
        entry = []
        for piece, *where in block:
            if isinstance(piece, tuple):
                mine, theirs, first, at = piece
                sources.append((len(pieces), len(pieces) + 1, first, at))
                pieces += [mine, theirs]
                n, half = PIECE, theirs.shape[1]
                joined += (jax.ShapeDtypeStruct((n, 2 * half, d), theirs.dtype),)
                group = 2 * half
            else:
                sources.append((len(pieces),))
                pieces.append(piece)
                n, group, _ = piece.shape
            entry.append((n, *where))
        plan.append(tuple(entry))
    plan = tuple(plan)
    shape = jax.ShapeDtypeStruct((layers, batch, hk, group * tp // 2), weights[0].dtype)
    n_alias = 0 if out is None else 2
    n_in = 3 + len(pieces)
    stage = stage_shape(weights, sum(n for n, *_ in plan[0]), group)
    before, before_entry, chunks = carry
    tok = sum(n for entry in plan for n, *_ in entry) * group
    outs = pl.pallas_call(
        functools.partial(project_kernel, plan, tuple(sources), len(pieces), (before_entry, chunks), n_alias, keep, keep_joined, unroll),
        out_shape=(shape, shape) + (stage,) * keep + joined * keep_joined,
        in_specs=[VMEM] * n_in + [ANY] * n_alias,
        out_specs=(ANY, ANY) + (VMEM,) * (keep + len(joined) * keep_joined),
        input_output_aliases={n_in + i: i for i in range(n_alias)},
        scratch_shapes=[pltpu.VMEM(stage.shape, stage.dtype)] * (not keep) + [pltpu.VMEM(j.shape, j.dtype) for j in joined * (not keep_joined)] + [
            pltpu.SemaphoreType.DMA((stage.shape[0], 2, len(plan[0]))),
            pltpu.SemaphoreType.DMA((stage.shape[0], 2, len(before_entry))),
        ],
        compiler_params=pltpu.CompilerParams(vmem_limit_bytes=5 * 2**20),
        cost_estimate=pl.CostEstimate(
            flops=2 * tok * d * hk * 2 * layers,
            bytes_accessed=2 * tok * (d + 2 * layers * hk),
            transcendentals=0,
        ),
    )(*weights, *pieces, before, *(out or ()))
    chunks = stage.shape[0]
    carry = (outs[2], plan[-1], tuple(range(0 if unroll else chunks - 1, chunks))) if keep else None
    return outs[:2], carry, outs[2 + keep:]


def solution(mesh):
    tp = mesh.shape["tp"]
    chips = tp // 2
    ring = [(i, (i + 2 - 4 * (i % 2)) % tp) for i in range(tp)]
    swap = [(i, i ^ 1) for i in range(tp)]

    def send(v, perm):
        return lax.ppermute(v, "tp", perm)

    def per_device(enc_out, norm_scale, w_key, w_value):
        layers, d, heads, k = w_key.shape
        batch = enc_out.shape[0]
        wk = w_key.reshape(layers, d, heads * k).transpose(0, 2, 1)
        wv = w_value.reshape(layers, d, heads * k).transpose(0, 2, 1)
        n = batch // PIECE
        h = n // 2
        seq = lambda i: (i % n) * PIECE

        state = {"out": None}

        def run(blocks, keep=True, keep_joined=True, unroll=False):
            state["out"], state["carry"], joined = project(weights, blocks, state["out"], state["carry"], batch, tp, keep, keep_joined, unroll)
            return joined

        def hold(*arrays):
            arrays, state["out"] = lax.optimization_barrier((arrays, state["out"]))
            return arrays if len(arrays) > 1 else arrays[0]

        ya = normalize_first(enc_out, norm_scale, 0, PIECE)
        na = send(ya, ring)
        yb = normalize_first(enc_out, norm_scale, PIECE, batch // 2 - PIECE)
        nb = send(yb, ring)
        other, slots, weights, stage = prepare(enc_out, norm_scale, (wk, wv), ya, yb)
        own = lambda i: ((0, seq(i)), (0, seq(i + h)))
        state["carry"] = (stage, tuple((PIECE, *own(i)) for i in range(2)), tuple(range(stage.shape[0])))
        nz = [send(v, ring) for v in other]
        n3 = send(slots[0], ring)
        run([[((yb, other[1], PIECE, 0), *own(2)), (slots[0], *own(3))], [(slots[1], *own(4)), (slots[2], *own(5))]], keep_joined=False)

        LEFT, RIGHT = chips - 1, 1
        near = lambda i: ((LEFT, seq(i)), (RIGHT, seq(i + h)))
        far = lambda i: ((2, seq(i)), (2, seq(i + h)))
        mine = lambda p, where: (p, *where)
        theirs = lambda q, where: (q, *where[::-1])

        pa, pb, z0 = hold(na, nb, nz[0])
        n4, n5 = send(slots[1], ring), send(slots[2], ring)
        p0, p1 = run([[mine((pa, z0, 0, 0), near(0)), mine((pb, z0, 0, PIECE), near(1))]])
        q0, q1 = send(p0, swap), send(p1, swap)
        z1 = hold(nz[1])
        p2, = run([[mine((pb, z1, PIECE, 0), near(2))]])
        q2 = send(p2, swap)
        run([[theirs(q0, near(0)), theirs(q1, near(1))]])
        p3 = hold(n3)
        q3 = send(p3, swap)
        run([[theirs(q2, near(2)), mine(p3, near(3))]])
        p4, p0, p1, p2 = hold(n4, p0, p1, p2)
        q4 = send(p4, swap)
        f0, f1, f2 = (send(p, ring) for p in (p0, p1, p2))
        run([[theirs(q3, near(3)), mine(p4, near(4))]])
        p5 = hold(n5)
        q5 = send(p5, swap)
        run([[theirs(q4, near(4)), mine(p5, near(5))]])
        run([[theirs(q5, near(5))]], unroll=True)
        for i, v in enumerate((f0, f1, f2)):
            p = hold(v)
            q = send(p, swap)
            run([[mine(p, far(i))]], unroll=i != 1)
            q = hold(q)
            run([[theirs(q, far(i))]], keep=i < 2, unroll=i == 2)
        out = state["out"]
        to_cache = lambda o: o.reshape(layers, batch, heads, k, -1).transpose(0, 1, 4, 2, 3)
        return to_cache(out[0]), to_cache(out[1])

    weight_spec = P(None, None, "tp", None)
    cache_spec = P(None, "dp", None, "tp", None)
    step = jax.shard_map(per_device, mesh=mesh, in_specs=(P("dp", "tp", None), P(None), weight_spec, weight_spec), out_specs=(cache_spec, cache_spec), check_vma=False)

    def program(*args):
        jax.eval_shape(step, *args)
        return step(*args)

    return program
```
